32 devices in a mesh: row: 4 (over z), col: 8 (over y, x, core).
Axes of the slice: x: 2, y: 2, z: 4, core: 2. Of those that a mesh axis runs over, the one named last changes fastest.
Arguments:
- prior: float32 [80, 30, 16384], P(None, None, ('row', 'col')), may hold values from -6 to 6
- ocean_mask: int32 [16384], P(('row', 'col')), may hold values from 0 to 1
- tile_order: int32 [32], replicated, may hold values from 0 to 31, each once
- obs_cell: int32 [4, 128], replicated, may hold values from 0 to 16383
- obs_stack: int32 [4, 128], replicated, may hold values from 0 to 29
- obs_values: float32 [4, 128], replicated, may hold values from -8 to 8
- window_start: int32 [4, 128], replicated, may hold values from 0 to 16383
- window_span: int32 [4, 128], replicated, may hold values from 1024 to 4096
- gain_mean: float32 [4, 128, 128], replicated, may hold values from -0.2 to 0.8
- gain_spread: float32 [4, 128, 128], replicated, may hold values from -0.2 to 0.4
Outputs:
- posterior: float32 [80, 30, 16384], P(None, None, ('row', 'col'))
The draws below stay inside these ranges and needn't reach their ends.
Inputs may be any that keep to these rules, and one draw needn't show every extreme that they name: `tile_order`: each curve tile appears once.
All inputs are finite; a program needn't handle non-finite values.
Results may differ from the reference program's by a relative error of at most 0.0001.
Values sent between devices are 32-bit elements; how exact they have to be, the bound alone decides.
A program may use at most 64 MiB of HBM per device.

```python
import jax
import jax.numpy as jnp
from jax import lax

MEMBERS = 80
STACK = 30
OBS = 128
BATCHES = 4
COL_DEV = 512
NCOL = 16384
N_ROW = 4
N_COL = 8


def draw_ocean_mask(key, part):
    key_level, key_cells = jax.random.split(jax.random.fold_in(key, 3))
    tiles_count = NCOL // COL_DEV
    levels = jax.random.randint(key_level, (tiles_count, 1), 0, 5)
    patches = jax.random.randint(key_cells, (tiles_count, COL_DEV // 16), 0, 4)
    ocean = (patches < levels).astype(jnp.int32)
    return jnp.repeat(ocean, 16, axis=1).reshape(NCOL)


def factor_draw(key, lowest, highest, off_scale):
    key_diag, key_off = jax.random.split(key)
    diagonal = jnp.exp(jax.random.uniform(key_diag, (BATCHES, OBS), jnp.float32, jnp.log(lowest), jnp.log(highest)))
    off_part = off_scale * jnp.clip(jax.random.normal(key_off, (BATCHES, OBS, OBS), jnp.float32), -6.0, 6.0)
    identity = jnp.eye(OBS, dtype=jnp.float32)
    return off_part * (1.0 - identity)[None] + diagonal[:, :, None] * identity[None]


def draw_gain_mean(key, part):
    return factor_draw(jax.random.fold_in(key, 11), 0.2, 0.8, 0.02)


def draw_gain_spread(key, part):
    return factor_draw(jax.random.fold_in(key, 17), 0.1, 0.4, 0.015)


def place_ends(array, own_key, smallest, high):
    extent = array.shape
    index_at = [jax.random.randint(jax.random.fold_in(own_key, axis), (), 0, extent[axis]) for axis in range(len(extent))]
    array = array.at[tuple(index_at)].set(smallest)
    longest = extent.index(max(extent))
    index_at[longest] = (index_at[longest] + 1) % extent[longest]
    return array.at[tuple(index_at)].set(high)


def block_levels(own_key, extent, shards, low, largest):
    def one(dim, parts):
        draws = jax.random.uniform(jax.random.fold_in(jax.random.fold_in(own_key, 6), dim), (parts,), jnp.float32, low / len(shards), largest / len(shards))
        return jnp.repeat(jnp.exp(draws), extent[dim] // parts).reshape((-1,) + (1,) * (len(extent) - dim - 1))

    factor_of = one(*shards[0])
    for cut in shards[1:]:
        factor_of = factor_of * one(*cut)
    return factor_of


def bell_draw(stream_key, shape, scale, bound, cuts=(), kind=jnp.bfloat16):
    gain = block_levels(stream_key, shape, cuts, -0.22, 0.18) if cuts else 1.0
    entries = jax.random.normal(stream_key, shape, jnp.float32) * scale * gain
    return jnp.minimum(jnp.maximum(entries, -bound), bound).astype(kind)


def setup_inputs(seed: int = 0) -> dict:
    streams_of = jax.random.split(jax.random.key(seed), 11)
    return {
        "prior": bell_draw(streams_of[0], (MEMBERS, STACK, NCOL), 1.0, 6.0, ((2, 32),), jnp.float32),
        "ocean_mask": draw_ocean_mask(jax.random.fold_in(streams_of[10], 71), 0),
        "tile_order": jax.random.permutation(streams_of[2], N_ROW * N_COL).astype(jnp.int32),
        "obs_cell": place_ends(jax.random.randint(streams_of[3], (BATCHES, OBS), 0, NCOL), jax.random.fold_in(streams_of[3], 1), 0, NCOL - 1).astype(jnp.int32),
        "obs_stack": place_ends(jax.random.randint(streams_of[4], (BATCHES, OBS), 0, STACK), jax.random.fold_in(streams_of[4], 1), 0, STACK - 1).astype(jnp.int32),
        "obs_values": bell_draw(streams_of[5], (BATCHES, OBS), 1.5, 8.0, (), jnp.float32),
        "window_start": place_ends(jax.random.randint(streams_of[6], (BATCHES, OBS), 0, NCOL), jax.random.fold_in(streams_of[6], 1), 0, NCOL - 1).astype(jnp.int32),
        "window_span": place_ends(jax.random.randint(streams_of[7], (BATCHES, OBS), NCOL // 16, NCOL // 4 + 1), jax.random.fold_in(streams_of[7], 1), NCOL // 16, (NCOL // 4 + 1) - 1).astype(jnp.int32),
        "gain_mean": draw_gain_mean(jax.random.fold_in(streams_of[10], 71), 0),
        "gain_spread": draw_gain_spread(jax.random.fold_in(streams_of[10], 71), 0),
    }


HIGHEST_PRECISION = lax.Precision.HIGHEST


def regress(section, anomalies, mean_weights, spread_weights, local_weight):
    members = section.shape[0]
    centre = jnp.mean(section, axis=0)
    spread = section - centre[None]
    covariance = jnp.einsum("msc,mp->scp", spread, anomalies, precision=HIGHEST_PRECISION) / (members - 1.0)
    gain_matrix = covariance * local_weight[None]
    increment = jnp.einsum("scp,p->sc", gain_matrix, mean_weights, precision=HIGHEST_PRECISION)
    change = jnp.einsum("scp,pm->msc", gain_matrix, spread_weights, precision=HIGHEST_PRECISION)
    return centre[None] + increment[None] + spread - change


def window_weight(places, ocean_flag, starts, extents):
    inside = (places[:, None] >= starts[None, :]) & (places[:, None] < starts[None, :] + extents[None, :])
    return ocean_flag[:, None] * inside.astype(ocean_flag.dtype)


def batch_weights(priors, observed, gain_mean, gain_spread):
    centre = jnp.mean(priors, axis=0)
    anomalies = priors - centre[None]
    mean_weights = jnp.dot(gain_mean, observed - centre, precision=HIGHEST_PRECISION)
    spread_weights = jnp.dot(gain_spread, anomalies.T, precision=HIGHEST_PRECISION)
    return anomalies, mean_weights, spread_weights


def reference(prior, ocean_mask, tile_order, obs_cell, obs_stack, obs_values, window_start, window_span, gain_mean, gain_spread):
    columns_all = prior.shape[2]
    storage = jnp.arange(columns_all, dtype=jnp.int32)
    places = (tile_order[storage // COL_DEV] * COL_DEV + storage % COL_DEV).astype(jnp.int32)
    inverse = jnp.argsort(tile_order).astype(jnp.int32)
    ocean_flag = ocean_mask.astype(prior.dtype)
    ensemble = prior
    for batch_number in range(BATCHES):
        cells = obs_cell[batch_number].astype(jnp.int32)
        holder = (inverse[cells // COL_DEV] * COL_DEV + cells % COL_DEV).astype(jnp.int32)
        flattened = ensemble.reshape(MEMBERS, -1)
        spots = (obs_stack[batch_number] * columns_all + holder).astype(jnp.int32)
        priors = jnp.take(flattened, spots, axis=1)
        anomalies, mean_weights, spread_weights = batch_weights(priors, obs_values[batch_number], gain_mean[batch_number], gain_spread[batch_number])
        starts = window_start[batch_number]
        extents = window_span[batch_number]

        def advance(loop_number, current):
            offset = (loop_number * COL_DEV).astype(jnp.int32)
            section = lax.dynamic_slice_in_dim(current, offset, COL_DEV, 2)
            weight = window_weight(lax.dynamic_slice_in_dim(places, offset, COL_DEV, 0), lax.dynamic_slice_in_dim(ocean_flag, offset, COL_DEV, 0), starts, extents)
            renewed = regress(section, anomalies, mean_weights, spread_weights, weight)
            return lax.dynamic_update_slice_in_dim(current, renewed, offset, 2)

        ensemble = lax.fori_loop(0, columns_all // COL_DEV, advance, ensemble)
    return ensemble
```

```python
import functools

import jax
import jax.numpy as jnp
from jax import lax
from jax.experimental import pallas as pl
from jax.experimental.pallas import tpu as pltpu
from jax.sharding import PartitionSpec as P

MESH = pl.DeviceIdType.MESH
NT = (((1,), (1,)), ((), ()))
SLOTS = 64
SIZES = (48, 80)


def device_number():
    return lax.axis_index("row") * lax.axis_size("col") + lax.axis_index("col")


def round_up(number, step):
    return (number + step - 1) // step * step


def extract_kernel(
    columns, rows, order_s, cell_s, stack_s, ocean_s, x_hbm, out_ref, found, buf, acc, sems
):
    batches, obs = cell_s.shape
    members = buf.shape[1]
    chunks, chunk_rows, _ = out_ref.shape
    base = order_s[device_number()] * columns
    acc[...] = jnp.zeros_like(acc)

    count = 0
    for batch in range(batches):

        def scan(j, count, batch=batch):
            found[count] = batch * obs + j
            local = cell_s[batch, j] - base
            here = jnp.logical_and(local >= 0, local < columns)
            return count + here.astype(jnp.int32)

        count = lax.fori_loop(0, obs, scan, count, unroll=32)
    lane = lax.broadcasted_iota(jnp.int32, (members, obs), 1)
    row = lax.broadcasted_iota(jnp.int32, (8, obs), 0)
    lane8 = lax.broadcasted_iota(jnp.int32, (8, obs), 1)

    def fetch(index, slot):
        b, j = index // obs, index % obs
        local = cell_s[b, j] - base
        tile = pl.multiple_of(local // 128 * 128, 128)
        return pltpu.make_async_copy(
            x_hbm.at[stack_s[b, j], :, pl.ds(tile, 128)], buf.at[slot], sems.at[slot]
        )

    def group(number, carry):
        first = number * SLOTS
        held = jnp.minimum(count - first, SLOTS)

        def start(slot, c):
            fetch(found[first + slot], slot).start()
            return c

        def finish(slot, c):
            index = found[first + slot]
            fetch(index, slot).wait()
            b, j = index // obs, index % obs
            local = cell_s[b, j] - base
            moved = pltpu.roll(buf[slot], (j - local % 128 + 128) % 128, axis=1)
            top = pl.multiple_of(b * rows, 8)
            acc[pl.ds(top, members), :] = jnp.where(
                lane == j, moved, acc[pl.ds(top, members), :]
            )
            flag = jnp.where(row == 0, ocean_s[local].astype(jnp.float32), 0.0)
            low = pl.multiple_of(top + members, 8)
            acc[pl.ds(low, 8), :] = jnp.where(lane8 == j, flag, acc[pl.ds(low, 8), :])
            return c

        lax.fori_loop(0, held, start, 0)
        lax.fori_loop(0, held, finish, 0)
        return carry

    lax.fori_loop(0, (count + SLOTS - 1) // SLOTS, group, 0)
    for chunk in range(chunks):
        out_ref[chunk] = acc[chunk * chunk_rows : (chunk + 1) * chunk_rows, :]


def exchange_kernel(part, out, landed, send_a, recv_a, send_b, recv_b):
    devices = part.shape[0]
    cols = lax.axis_size("col")
    me = device_number()

    def peer(step):
        return lax.rem(me + step, devices)

    def place(number):
        return (number // cols, lax.rem(number, cols))

    barrier = pltpu.get_barrier_semaphore()

    def greet(step, c):
        pl.semaphore_signal(barrier, inc=1, device_id=place(peer(step)), device_id_type=MESH)
        return c

    lax.fori_loop(1, devices, greet, 0)
    pl.semaphore_wait(barrier, devices - 1)

    def scatter(other, slot):
        return pltpu.make_async_remote_copy(
            src_ref=part.at[other],
            dst_ref=landed.at[slot],
            send_sem=send_a.at[other],
            recv_sem=recv_a.at[slot],
            device_id=place(other),
            device_id_type=MESH,
        )

    def gather(other, slot):
        return pltpu.make_async_remote_copy(
            src_ref=out.at[me],
            dst_ref=out.at[slot],
            send_sem=send_b.at[other],
            recv_sem=recv_b.at[slot],
            device_id=place(other),
            device_id_type=MESH,
        )

    def each(act):
        def step(number, c):
            act(peer(number))
            return c

        lax.fori_loop(1, devices, step, 0)

    each(lambda other: scatter(other, me).start())
    landed[me] = part[me]
    each(lambda other: scatter(other, other).wait_recv())
    out[me] = jnp.sum(landed[...], axis=0)
    each(lambda other: gather(other, me).start())
    each(lambda other: gather(other, other).wait_recv())
    each(lambda other: scatter(other, me).wait_send())
    each(lambda other: gather(other, me).wait_send())


def split(values):
    high = values.astype(jnp.bfloat16)
    low = (values - high.astype(jnp.float32)).astype(jnp.bfloat16)
    return high, low


def triple(values, axis):
    high, low = split(values)
    return jnp.concatenate([high, low, high], axis=axis)


def product(left, right):
    high, low = split(left)
    return lax.dot_general(
        jnp.concatenate([high, high, low], axis=1),
        triple(right, 1),
        NT,
        preferred_element_type=jnp.float32,
    )


def update_kernel(
    rows,
    order_s,
    ocean_ref,
    cell_ref,
    start_ref,
    span_ref,
    value_ref,
    mean_ref,
    spread_ref,
    shared_ref,
    x_hbm,
    y_hbm,
    xt,
    flat,
    side_a,
    side_d,
    lhs_a,
    lhs_d,
    weight,
    sem_in,
    sem_out,
):
    stack, members, columns = xt.shape
    batches, obs = cell_ref.shape
    chunks, chunk_rows, _ = shared_ref.shape

    def incoming(v):
        return pltpu.make_async_copy(x_hbm.at[v], xt.at[v], sem_in.at[v])

    def outgoing(v):
        return pltpu.make_async_copy(xt.at[v], y_hbm.at[v], sem_out.at[v])

    def begin(v, c):
        incoming(v).start()
        return c

    lax.fori_loop(0, stack, begin, 0)

    for chunk in range(chunks):
        flat[chunk * chunk_rows : (chunk + 1) * chunk_rows, :] = shared_ref[chunk]
    base = (order_s[device_number()] * columns).astype(jnp.float32)
    places = base + lax.broadcasted_iota(jnp.int32, (1, columns), 1).astype(jnp.float32)
    ocean = ocean_ref[...].astype(jnp.float32)
    cells = cell_ref[...].astype(jnp.float32)
    starts = start_ref[...].astype(jnp.float32)
    ends = (start_ref[...] + span_ref[...]).astype(jnp.float32)
    priors = [flat[b * rows : b * rows + members, :] for b in range(batches)]
    flags = [flat[b * rows + members : b * rows + members + 1, :] for b in range(batches)]
    scale = 1.0 / (members - 1.0)
    meets = jnp.logical_and(starts < base + columns, ends > base).astype(jnp.float32)
    before = lax.broadcasted_iota(jnp.int32, (obs, obs), 0) < lax.broadcasted_iota(
        jnp.int32, (obs, obs), 1
    )
    ranks = jnp.dot(
        jnp.concatenate([meets, jnp.zeros((16 - batches, obs), jnp.float32)], axis=0).astype(
            jnp.bfloat16
        ),
        before.astype(jnp.bfloat16),
        preferred_element_type=jnp.float32,
    )
    most = jnp.max(jnp.sum(meets, axis=1)).astype(jnp.int32)

    for b in range(batches):
        now = priors[b]
        centre = jnp.mean(now, axis=0, keepdims=True)
        anomalies = now - centre
        innovation = jnp.broadcast_to(value_ref[b : b + 1, :] - centre, (16, obs))
        mean_weights = product(innovation, mean_ref[b])[0:1]
        delta = mean_weights - product(anomalies, spread_ref[b])
        scaled = anomalies * scale
        high = scaled.astype(jnp.bfloat16).astype(jnp.float32)
        stacked = jnp.concatenate([high, high, scaled - high], axis=0)
        side_a[b] = stacked.astype(jnp.bfloat16)
        d_high, d_low = split(delta)
        side_d[b, 0] = d_high
        side_d[b, 1] = d_low
        if b + 1 < batches:
            start_of = jnp.transpose(jnp.broadcast_to(starts[b : b + 1], (128, obs)))[:, 0:1]
            end_of = jnp.transpose(jnp.broadcast_to(ends[b : b + 1], (128, obs)))[:, 0:1]
            later = jnp.concatenate(priors[b + 1 :], axis=1)
            cell_row = jnp.concatenate([cells[a : a + 1] for a in range(b + 1, batches)], axis=1)
            flag_row = jnp.concatenate(flags[b + 1 :], axis=1)
            inside = jnp.where(
                jnp.logical_and(cell_row >= start_of, cell_row < end_of), flag_row, 0.0
            )
            gain = inside * jnp.dot(
                jnp.transpose(stacked).astype(jnp.bfloat16),
                triple(later, 0),
                preferred_element_type=jnp.float32,
            )
            later = later + jnp.dot(
                jnp.concatenate([d_high, d_high, d_low], axis=1),
                triple(gain, 0),
                preferred_element_type=jnp.float32,
            )
            for a in range(b + 1, batches):
                priors[a] = later[:, (a - b - 1) * obs : (a - b) * obs]

    together = max(k for k in range(1, 7) if stack % k == 0)

    def sweep_with(kept):
        slot = lax.broadcasted_iota(jnp.int32, (kept, obs), 0).astype(jnp.float32)
        for b in range(batches):
            chosen = jnp.logical_and(slot == ranks[b : b + 1], meets[b : b + 1] > 0.0)
            start_of = jnp.sum(jnp.where(chosen, starts[b : b + 1], 0.0), axis=1, keepdims=True)
            end_of = jnp.sum(jnp.where(chosen, ends[b : b + 1], 0.0), axis=1, keepdims=True)
            weight[b, 0:kept] = jnp.where(
                jnp.logical_and(places >= start_of, places < end_of), ocean, 0.0
            )
            pick = chosen.astype(jnp.bfloat16)
            none = jnp.zeros_like(pick)
            lhs_a[b, 0:kept] = lax.dot_general(
                pick, side_a[b], NT, preferred_element_type=jnp.float32
            ).astype(jnp.bfloat16)
            lhs_d[b, :, 0 : 3 * kept] = (
                lax.dot_general(
                    side_d[b, 0],
                    jnp.concatenate([pick, pick, none], axis=0),
                    NT,
                    preferred_element_type=jnp.float32,
                )
                + lax.dot_general(
                    side_d[b, 1],
                    jnp.concatenate([none, none, pick], axis=0),
                    NT,
                    preferred_element_type=jnp.float32,
                )
            ).astype(jnp.bfloat16)

        def sweep(number, c):
            levels = [number * together + k for k in range(together)]
            for v in levels:
                incoming(v).wait()
            values = [xt[v] for v in levels]
            for b in range(batches):
                gains = []
                for k in range(together):
                    gain = weight[b, 0:kept] * jnp.dot(
                        lhs_a[b, 0:kept],
                        triple(values[k], 0),
                        preferred_element_type=jnp.float32,
                    )
                    gains.append(triple(gain, 0))
                for k in range(together):
                    values[k] = values[k] + jnp.dot(
                        lhs_d[b, :, 0 : 3 * kept], gains[k], preferred_element_type=jnp.float32
                    )
            for k in range(together):
                xt[levels[k]] = values[k]
            for v in levels:
                outgoing(v).start()
            return c

        lax.fori_loop(0, stack // together, sweep, 0)

    sizes = [kept for kept in SIZES if kept < obs] + [obs]
    for low, kept in zip([-1] + sizes[:-1], sizes):
        pl.when(jnp.logical_and(most > low, most <= kept))(functools.partial(sweep_with, kept))

    def end(v, c):
        outgoing(v).wait()
        return c

    lax.fori_loop(0, stack, end, 0)


def per_device(
    prior,
    ocean_mask,
    tile_order,
    obs_cell,
    obs_stack,
    obs_values,
    window_start,
    window_span,
    gain_mean,
    gain_spread,
):
    members, stack, columns = prior.shape
    batches, obs = obs_cell.shape
    devices = tile_order.shape[0]
    rows = members + 8
    chunk_rows = -(-batches * rows // devices)
    smem = pl.BlockSpec(memory_space=pltpu.SMEM)
    vmem = pl.BlockSpec(memory_space=pltpu.VMEM)
    hbm = pl.BlockSpec(memory_space=pl.ANY)
    shared_shape = jax.ShapeDtypeStruct((devices, chunk_rows, obs), jnp.float32)
    flat_rows = round_up(devices * chunk_rows, 8)

    levels = jnp.transpose(prior, (1, 0, 2))
    part = pl.pallas_call(
        functools.partial(extract_kernel, columns, rows),
        out_shape=shared_shape,
        in_specs=[smem, smem, smem, smem, hbm],
        out_specs=vmem,
        scratch_shapes=[
            pltpu.SMEM((batches * obs + 1,), jnp.int32),
            pltpu.VMEM((SLOTS, members, 128), jnp.float32),
            pltpu.VMEM((flat_rows, obs), jnp.float32),
            pltpu.SemaphoreType.DMA((SLOTS,)),
        ],
        name="extract",
    )(tile_order, obs_cell, obs_stack, ocean_mask, levels)

    shared = pl.pallas_call(
        exchange_kernel,
        out_shape=shared_shape,
        in_specs=[vmem],
        out_specs=vmem,
        scratch_shapes=[pltpu.VMEM((devices, chunk_rows, obs), jnp.float32)]
        + [pltpu.SemaphoreType.DMA((devices,))] * 4,
        compiler_params=pltpu.CompilerParams(collective_id=0, has_side_effects=True),
        name="exchange",
    )(part)

    updated = pl.pallas_call(
        functools.partial(update_kernel, rows),
        out_shape=jax.ShapeDtypeStruct(levels.shape, levels.dtype),
        in_specs=[smem] + [vmem] * 8 + [hbm],
        out_specs=hbm,
        scratch_shapes=[
            pltpu.VMEM((stack, members, columns), jnp.float32),
            pltpu.VMEM((flat_rows, obs), jnp.float32),
            pltpu.VMEM((batches, 3 * members, obs), jnp.bfloat16),
            pltpu.VMEM((batches, 2, members, obs), jnp.bfloat16),
            pltpu.VMEM((batches, obs, 3 * members), jnp.bfloat16),
            pltpu.VMEM((batches, members, 3 * obs), jnp.bfloat16),
            pltpu.VMEM((batches, obs, columns), jnp.float32),
            pltpu.SemaphoreType.DMA((stack,)),
            pltpu.SemaphoreType.DMA((stack,)),
        ],
        name="update",
    )(
        tile_order,
        ocean_mask.reshape(1, columns),
        obs_cell,
        window_start,
        window_span,
        obs_values,
        gain_mean,
        gain_spread,
        shared,
        levels,
    )
    return jnp.transpose(updated, (1, 0, 2))


def solution(mesh):
    in_specs = (P(None, None, ("row", "col")), P(("row", "col"))) + (P(),) * 8
    return jax.shard_map(
        per_device,
        mesh=mesh,
        in_specs=in_specs,
        out_specs=P(None, None, ("row", "col")),
        check_vma=False,
    )
```

```python
import functools
import math

import jax
import jax.numpy as jnp
from jax import lax
from jax.experimental import pallas as pl
from jax.experimental.pallas import tpu as pltpu
from jax.sharding import PartitionSpec as P

MESH = pl.DeviceIdType.MESH
NT = (((1,), (1,)), ((), ()))
SIZES = (48, 80)


def device_number():
    return lax.axis_index("row") * lax.axis_size("col") + lax.axis_index("col")


def round_up(number, step):
    return (number + step - 1) // step * step


def mate(index, step, size):
    if size & (size - 1):
        return lax.rem(index + step, size)
    bit = 1
    while bit <= step:
        if step & bit:
            index = index + bit - 2 * bit * (index // bit % 2)
        bit *= 2
    return index


def column_of(row):
    width = row.shape[1]
    return jnp.transpose(jnp.broadcast_to(row, (128, width)))[:, 0:1]


def gather_plan(gath, sends, receives):
    rows, cols = lax.axis_size("row"), lax.axis_size("col")
    plane = cols // 2
    row, col = lax.axis_index("row"), lax.axis_index("col")
    core, chip = lax.rem(col, 2), col // 2
    other = (row, chip * 2 + 1 - core)

    def near(step):
        return (row, mate(chip, step, plane) * 2 + core)

    def far(step):
        return (mate(row, step, rows), col)

    peers = [far(step) for step in range(1, rows)] + [near(step) for step in range(1, plane)] + [other]

    def slot(row_step, chip_step, twin):
        return (
            mate(row, row_step, rows) * cols
            + mate(chip, chip_step, plane) * 2
            + (1 - core if twin else core)
        )

    started = []

    def send(number, place):
        copy = pltpu.make_async_remote_copy(
            src_ref=gath.at[number],
            dst_ref=gath.at[number],
            send_sem=sends.at[len(started)],
            recv_sem=receives.at[number],
            device_id=place,
            device_id_type=MESH,
        )
        copy.start()
        started.append(copy)

    def arrive(number):
        pltpu.make_async_remote_copy(
            src_ref=gath.at[number],
            dst_ref=gath.at[number],
            send_sem=sends.at[0],
            recv_sem=receives.at[number],
            device_id=other,
            device_id_type=MESH,
        ).wait_recv()

    def spread(number):
        for step in reversed(range(1, plane)):
            send(number, near(step))
        send(number, other)

    def begin():
        mine = slot(0, 0, False)
        for step in reversed(range(1, rows)):
            send(mine, far(step))
        spread(mine)

    def finish():
        for step in range(1, rows):
            number = slot(step, 0, False)
            arrive(number)
            spread(number)
        for row_step in range(rows):
            for step in range(1, plane):
                number = slot(row_step, step, False)
                arrive(number)
                send(number, other)
        for row_step in range(rows):
            for step in range(plane):
                arrive(slot(row_step, step, True))

    def drain():
        for copy in started:
            copy.wait_send()

    return peers, begin, finish, drain


def share_kernel(
    round_s,
    ocean_s,
    order_s,
    order_ref,
    cell_ref,
    stack_ref,
    x_hbm,
    flat_ref,
    rounds_s,
    xt,
    list_v,
    list_s,
    gath,
    place_t,
    sem_in,
    sem_list,
    sends,
    receives,
):
    stack, members, columns = x_hbm.shape
    batches, obs = cell_ref.shape
    devices, cap, lanes = gath.shape
    groups = columns // lanes
    me = device_number()
    state = [
        pltpu.make_async_copy(
            x_hbm.at[:, :, g * lanes : (g + 1) * lanes],
            xt.at[g * stack : (g + 1) * stack],
            sem_in.at[g],
        )
        for g in range(groups)
    ]
    for copy in state:
        copy.start()
    peers, begin, finish, drain = gather_plan(gath, sends, receives)
    barrier = pltpu.get_barrier_semaphore()
    for place in peers:
        pl.semaphore_signal(barrier, inc=1, device_id=place, device_id_type=MESH)

    local = cell_ref[...] - order_s[me] * columns
    here = jnp.logical_and(local >= 0, local < columns)
    ahead = here.astype(jnp.int32)
    total = ahead
    along = lax.broadcasted_iota(jnp.int32, (batches, obs), 1)
    step = 1
    while step < obs:
        ahead = ahead + jnp.where(along >= step, pltpu.roll(ahead, step, axis=1), 0)
        total = total + pltpu.roll(total, step, axis=1)
        step *= 2
    code = stack_ref[...] * columns + local
    slot_of = lax.broadcasted_iota(jnp.int32, (cap, obs), 0) + round_s[0] * cap + 1
    codes = jnp.zeros((cap, obs), jnp.int32)
    earlier = jnp.zeros((1, obs), jnp.int32)
    for b in range(batches):
        mine = jnp.where(here[b : b + 1], ahead[b : b + 1] + earlier, 0)
        codes = codes + jnp.where(mine == slot_of, code[b : b + 1], 0)
        earlier = earlier + total[b : b + 1]
    step = 1
    while step < obs:
        codes = codes + pltpu.roll(codes, step, axis=1)
        step *= 2
    list_v[...] = codes
    listing = pltpu.make_async_copy(list_v, list_s, sem_list)
    listing.start()

    first = (round_s[0] * cap).astype(jnp.float32)
    number = lax.broadcasted_iota(jnp.int32, (devices, obs), 0).astype(jnp.float32)
    square = (devices, devices)
    same = lax.broadcasted_iota(jnp.int32, square, 0) == lax.broadcasted_iota(jnp.int32, square, 1)
    order = jnp.sum(
        jnp.where(same, order_ref[...].astype(jnp.float32), 0.0), axis=1, keepdims=True
    )
    before = lax.broadcasted_iota(jnp.int32, (obs, obs), 0) < lax.broadcasted_iota(
        jnp.int32, (obs, obs), 1
    )
    before = before.astype(jnp.bfloat16)
    count = jnp.zeros((devices, 1), jnp.float32)
    slots = []
    for b in range(batches):
        cells = cell_ref[b : b + 1, :].astype(jnp.float32)
        tile = jnp.floor((cells + 0.5) / columns)
        holds = (order == tile).astype(jnp.float32)
        rank = count + jnp.dot(
            holds.astype(jnp.bfloat16), before, preferred_element_type=jnp.float32
        )
        count = count + jnp.sum(holds, axis=1, keepdims=True)
        rank = jnp.sum(holds * rank, axis=0, keepdims=True) - first
        holder = jnp.sum(holds * number, axis=0, keepdims=True)
        now = jnp.logical_and(rank >= 0.0, rank < cap)
        slots.append(jnp.where(now, holder * cap + rank, -1.0))
    rounds_s[0] = jnp.max(jnp.floor((count + (cap - 0.5)) / cap)).astype(jnp.int32)
    listing.wait()
    for copy in state:
        copy.wait()

    lane = lax.broadcasted_iota(jnp.int32, (members, lanes), 1)
    row8 = lax.broadcasted_iota(jnp.int32, (8, lanes), 0)
    lane8 = lax.broadcasted_iota(jnp.int32, (8, lanes), 1)

    def pick(k, carry):
        held, flags = carry
        code = list_s[k, 0]
        level = lax.div(code, columns)
        local = code - level * columns
        group = lax.div(local, lanes)
        block = xt[group * stack + level]
        moved = pltpu.roll(block, lax.rem(k - (local - group * lanes) + lanes, lanes), axis=1)
        held = jnp.where(lane == k, moved, held)
        flag = jnp.where(row8 == 0, ocean_s[local].astype(jnp.float32), 0.0)
        return held, jnp.where(lane8 == k, flag, flags)

    held, flags = lax.fori_loop(
        0,
        cap,
        pick,
        (jnp.zeros((members, lanes), jnp.float32), jnp.zeros((8, lanes), jnp.float32)),
        unroll=8,
    )
    rest = jnp.zeros((lanes - members - 8, lanes), jnp.float32)
    gath[me] = jnp.transpose(jnp.concatenate([held, flags, rest], axis=0))[0:cap, :]

    pl.semaphore_wait(barrier, len(peers))
    begin()
    at = lax.broadcasted_iota(jnp.int32, (obs, devices * cap), 1).astype(jnp.float32)
    for b in range(batches):
        place_t[b * obs : (b + 1) * obs, :] = (column_of(slots[b]) == at).astype(jnp.bfloat16)
    finish()

    got = jnp.concatenate([gath[k] for k in range(devices)], axis=0)
    high, low = split(got)
    rest = (got - high.astype(jnp.float32) - low.astype(jnp.float32)).astype(jnp.bfloat16)
    parts = jnp.dot(
        place_t[...],
        jnp.concatenate([high, low, rest], axis=1),
        preferred_element_type=jnp.float32,
    )
    placed = parts[:, 0:lanes] + parts[:, lanes : 2 * lanes] + parts[:, 2 * lanes :]
    for b in range(batches):
        flat_ref[b] = jnp.transpose(placed[b * obs : (b + 1) * obs, :])
    drain()


def split(values):
    high = values.astype(jnp.bfloat16)
    low = (values - high.astype(jnp.float32)).astype(jnp.bfloat16)
    return high, low


def triple(values, axis):
    high, low = split(values)
    return jnp.concatenate([high, low, high], axis=axis)


def product(left, right):
    high, low = split(left)
    return lax.dot_general(
        jnp.concatenate([high, high, low], axis=1),
        triple(right, 1),
        NT,
        preferred_element_type=jnp.float32,
    )


def update_kernel(
    order_s,
    ocean_ref,
    cell_ref,
    start_ref,
    span_ref,
    value_ref,
    mean_ref,
    spread_ref,
    shared_ref,
    x_hbm,
    y_hbm,
    xt,
    side_a,
    side_d,
    lhs_a,
    lhs_d,
    weight,
    sem_in,
    sem_out,
):
    stack, members, columns = xt.shape
    batches, obs = cell_ref.shape

    def incoming(v):
        return pltpu.make_async_copy(x_hbm.at[v], xt.at[v], sem_in.at[v])

    def outgoing(v):
        return pltpu.make_async_copy(xt.at[v], y_hbm.at[v], sem_out.at[v])

    def begin(v, c):
        incoming(v).start()
        return c

    lax.fori_loop(0, stack, begin, 0)

    base = (order_s[device_number()] * columns).astype(jnp.float32)
    places = base + lax.broadcasted_iota(jnp.int32, (1, columns), 1).astype(jnp.float32)
    ocean = ocean_ref[...].astype(jnp.float32)
    cells = cell_ref[...].astype(jnp.float32)
    starts = start_ref[...].astype(jnp.float32)
    ends = (start_ref[...] + span_ref[...]).astype(jnp.float32)
    priors = [shared_ref[b, 0:members, :] for b in range(batches)]
    flags = [shared_ref[b, members : members + 1, :] for b in range(batches)]
    scale = 1.0 / (members - 1.0)
    meets = jnp.logical_and(starts < base + columns, ends > base).astype(jnp.float32)
    before = lax.broadcasted_iota(jnp.int32, (obs, obs), 0) < lax.broadcasted_iota(
        jnp.int32, (obs, obs), 1
    )
    ranks = jnp.dot(
        jnp.concatenate([meets, jnp.zeros((16 - batches, obs), jnp.float32)], axis=0).astype(
            jnp.bfloat16
        ),
        before.astype(jnp.bfloat16),
        preferred_element_type=jnp.float32,
    )
    most = jnp.max(jnp.sum(meets, axis=1)).astype(jnp.int32)

    for b in range(batches):
        now = priors[b]
        centre = jnp.mean(now, axis=0, keepdims=True)
        anomalies = now - centre
        innovation = jnp.broadcast_to(value_ref[b : b + 1, :] - centre, (16, obs))
        mean_weights = product(innovation, mean_ref[b])[0:1]
        delta = mean_weights - product(anomalies, spread_ref[b])
        scaled = anomalies * scale
        high = scaled.astype(jnp.bfloat16).astype(jnp.float32)
        stacked = jnp.concatenate([high, high, scaled - high], axis=0)
        side_a[b] = stacked.astype(jnp.bfloat16)
        d_high, d_low = split(delta)
        side_d[b, 0] = d_high
        side_d[b, 1] = d_low
        if b + 1 < batches:
            start_of = jnp.transpose(jnp.broadcast_to(starts[b : b + 1], (128, obs)))[:, 0:1]
            end_of = jnp.transpose(jnp.broadcast_to(ends[b : b + 1], (128, obs)))[:, 0:1]
            later = jnp.concatenate(priors[b + 1 :], axis=1)
            cell_row = jnp.concatenate([cells[a : a + 1] for a in range(b + 1, batches)], axis=1)
            flag_row = jnp.concatenate(flags[b + 1 :], axis=1)
            inside = jnp.where(
                jnp.logical_and(cell_row >= start_of, cell_row < end_of), flag_row, 0.0
            )
            gain = inside * jnp.dot(
                jnp.transpose(stacked).astype(jnp.bfloat16),
                triple(later, 0),
                preferred_element_type=jnp.float32,
            )
            later = later + jnp.dot(
                jnp.concatenate([d_high, d_high, d_low], axis=1),
                triple(gain, 0),
                preferred_element_type=jnp.float32,
            )
            for a in range(b + 1, batches):
                priors[a] = later[:, (a - b - 1) * obs : (a - b) * obs]

    together = max(k for k in range(1, 7) if stack % k == 0)

    def sweep_with(kept):
        slot = lax.broadcasted_iota(jnp.int32, (kept, obs), 0).astype(jnp.float32)
        for b in range(batches):
            chosen = jnp.logical_and(slot == ranks[b : b + 1], meets[b : b + 1] > 0.0)
            start_of = jnp.sum(jnp.where(chosen, starts[b : b + 1], 0.0), axis=1, keepdims=True)
            end_of = jnp.sum(jnp.where(chosen, ends[b : b + 1], 0.0), axis=1, keepdims=True)
            weight[b, 0:kept] = jnp.where(
                jnp.logical_and(places >= start_of, places < end_of), ocean, 0.0
            )
            pick = chosen.astype(jnp.bfloat16)
            none = jnp.zeros_like(pick)
            lhs_a[b, 0:kept] = lax.dot_general(
                pick, side_a[b], NT, preferred_element_type=jnp.float32
            ).astype(jnp.bfloat16)
            lhs_d[b, :, 0 : 3 * kept] = (
                lax.dot_general(
                    side_d[b, 0],
                    jnp.concatenate([pick, pick, none], axis=0),
                    NT,
                    preferred_element_type=jnp.float32,
                )
                + lax.dot_general(
                    side_d[b, 1],
                    jnp.concatenate([none, none, pick], axis=0),
                    NT,
                    preferred_element_type=jnp.float32,
                )
            ).astype(jnp.bfloat16)

        def sweep(number, c):
            levels = [number * together + k for k in range(together)]
            for v in levels:
                incoming(v).wait()
            values = [xt[v] for v in levels]
            for b in range(batches):
                gains = []
                for k in range(together):
                    gain = weight[b, 0:kept] * jnp.dot(
                        lhs_a[b, 0:kept],
                        triple(values[k], 0),
                        preferred_element_type=jnp.float32,
                    )
                    gains.append(triple(gain, 0))
                for k in range(together):
                    values[k] = values[k] + jnp.dot(
                        lhs_d[b, :, 0 : 3 * kept], gains[k], preferred_element_type=jnp.float32
                    )
            for k in range(together):
                xt[levels[k]] = values[k]
            for v in levels:
                outgoing(v).start()
            return c

        lax.fori_loop(0, stack // together, sweep, 0)

    sizes = [kept for kept in SIZES if kept < obs] + [obs]
    for low, kept in zip([-1] + sizes[:-1], sizes):
        pl.when(jnp.logical_and(most > low, most <= kept))(functools.partial(sweep_with, kept))

    def end(v, c):
        outgoing(v).wait()
        return c

    lax.fori_loop(0, stack, end, 0)


def per_device(
    prior,
    ocean_mask,
    tile_order,
    obs_cell,
    obs_stack,
    obs_values,
    window_start,
    window_span,
    gain_mean,
    gain_spread,
):
    members, stack, columns = prior.shape
    batches, obs = obs_cell.shape
    devices = tile_order.shape[0]
    mean = -(-batches * obs // devices)
    cap = min(round_up(mean + 4 * math.isqrt(mean), 8), 128)
    smem = pl.BlockSpec(memory_space=pltpu.SMEM)
    vmem = pl.BlockSpec(memory_space=pltpu.VMEM)
    hbm = pl.BlockSpec(memory_space=pl.ANY)

    levels = jnp.transpose(prior, (1, 0, 2))

    def share(number):
        return pl.pallas_call(
            share_kernel,
            out_shape=(
                jax.ShapeDtypeStruct((batches, 128, obs), jnp.float32),
                jax.ShapeDtypeStruct((1,), jnp.int32),
            ),
            in_specs=[smem, smem, smem, vmem, vmem, vmem, hbm],
            out_specs=(vmem, smem),
            scratch_shapes=[
                pltpu.VMEM((columns // 128 * stack, members, 128), jnp.float32),
                pltpu.VMEM((cap, obs), jnp.int32),
                pltpu.SMEM((cap, obs), jnp.int32),
                pltpu.VMEM((devices, cap, 128), jnp.float32),
                pltpu.VMEM((batches * obs, devices * cap), jnp.bfloat16),
                pltpu.SemaphoreType.DMA((columns // 128,)),
                pltpu.SemaphoreType.DMA,
                pltpu.SemaphoreType.DMA((devices,)),
                pltpu.SemaphoreType.DMA((devices,)),
            ],
            compiler_params=pltpu.CompilerParams(collective_id=0, has_side_effects=True),
            name="share",
        )(number, ocean_mask, tile_order, tile_order.reshape(1, devices), obs_cell, obs_stack, levels)

    shared, rounds = share(jnp.zeros((1,), jnp.int32))
    _, shared = lax.while_loop(
        lambda carry: carry[0] < rounds[0],
        lambda carry: (carry[0] + 1, carry[1] + share(carry[0].reshape(1))[0]),
        (jnp.int32(1), shared),
    )

    updated = pl.pallas_call(
        update_kernel,
        out_shape=jax.ShapeDtypeStruct(levels.shape, levels.dtype),
        in_specs=[smem] + [vmem] * 8 + [hbm],
        out_specs=hbm,
        scratch_shapes=[
            pltpu.VMEM((stack, members, columns), jnp.float32),
            pltpu.VMEM((batches, 3 * members, obs), jnp.bfloat16),
            pltpu.VMEM((batches, 2, members, obs), jnp.bfloat16),
            pltpu.VMEM((batches, obs, 3 * members), jnp.bfloat16),
            pltpu.VMEM((batches, members, 3 * obs), jnp.bfloat16),
            pltpu.VMEM((batches, obs, columns), jnp.float32),
            pltpu.SemaphoreType.DMA((stack,)),
            pltpu.SemaphoreType.DMA((stack,)),
        ],
        name="update",
    )(
        tile_order,
        ocean_mask.reshape(1, columns),
        obs_cell,
        window_start,
        window_span,
        obs_values,
        gain_mean,
        gain_spread,
        shared,
        levels,
    )
    return jnp.transpose(updated, (1, 0, 2))


def solution(mesh):
    in_specs = (P(None, None, ("row", "col")), P(("row", "col"))) + (P(),) * 8
    return jax.shard_map(
        per_device,
        mesh=mesh,
        in_specs=in_specs,
        out_specs=P(None, None, ("row", "col")),
        check_vma=False,
    )
```

```python
import functools
import math

import jax
import jax.numpy as jnp
from jax import lax
from jax.experimental import pallas as pl
from jax.experimental.pallas import tpu as pltpu
from jax.sharding import PartitionSpec as P

MESH = pl.DeviceIdType.MESH
NT = (((1,), (1,)), ((), ()))
SIZES = (48, 80)


def device_number():
    return lax.axis_index("row") * lax.axis_size("col") + lax.axis_index("col")


def round_up(number, step):
    return (number + step - 1) // step * step


def mate(index, step, size):
    if size & (size - 1):
        return lax.rem(index + step, size)
    bit = 1
    while bit <= step:
        if step & bit:
            index = index + bit - 2 * bit * (index // bit % 2)
        bit *= 2
    return index


def most_levels(stack, limit):
    return max(k for k in range(1, limit + 1) if stack % k == 0)


def column_of(row):
    width = row.shape[1]
    return jnp.transpose(jnp.broadcast_to(row, (128, width)))[:, 0:1]


def gather_plan(gath, sends, receives):
    rows, cols = lax.axis_size("row"), lax.axis_size("col")
    plane = cols // 2
    row, col = lax.axis_index("row"), lax.axis_index("col")
    core, chip = lax.rem(col, 2), col // 2
    other = (row, chip * 2 + 1 - core)

    def near(step):
        return (row, mate(chip, step, plane) * 2 + core)

    def far(step):
        return (mate(row, step, rows), col)

    peers = [far(step) for step in range(1, rows)] + [near(step) for step in range(1, plane)] + [other]

    def slot(row_step, chip_step, twin):
        return (
            mate(row, row_step, rows) * cols
            + mate(chip, chip_step, plane) * 2
            + (1 - core if twin else core)
        )

    started = []

    def send(number, place):
        copy = pltpu.make_async_remote_copy(
            src_ref=gath.at[number],
            dst_ref=gath.at[number],
            send_sem=sends.at[len(started)],
            recv_sem=receives.at[number],
            device_id=place,
            device_id_type=MESH,
        )
        copy.start()
        started.append(copy)

    def arrive(number):
        pltpu.make_async_remote_copy(
            src_ref=gath.at[number],
            dst_ref=gath.at[number],
            send_sem=sends.at[0],
            recv_sem=receives.at[number],
            device_id=other,
            device_id_type=MESH,
        ).wait_recv()

    def spread(number):
        for step in reversed(range(1, plane)):
            send(number, near(step))
        send(number, other)

    def begin():
        mine = slot(0, 0, False)
        for step in reversed(range(1, rows)):
            send(mine, far(step))
        spread(mine)

    def finish():
        for step in range(1, rows):
            number = slot(step, 0, False)
            arrive(number)
            spread(number)
        for row_step in range(rows):
            for step in range(1, plane):
                number = slot(row_step, step, False)
                arrive(number)
                send(number, other)
        for row_step in range(rows):
            for step in range(plane):
                arrive(slot(row_step, step, True))

    def drain():
        for copy in started:
            copy.wait_send()

    return peers, begin, finish, drain


def share_kernel(
    round_s,
    ocean_s,
    order_s,
    order_ref,
    cell_ref,
    stack_ref,
    x_hbm,
    flat_ref,
    rounds_s,
    xt,
    list_v,
    list_s,
    gath,
    place_t,
    sem_in,
    sem_list,
    sends,
    receives,
):
    stack, members, columns = x_hbm.shape
    batches, obs = cell_ref.shape
    devices, cap, lanes = gath.shape
    groups = columns // lanes
    me = device_number()
    state = [
        pltpu.make_async_copy(
            x_hbm.at[:, :, g * lanes : (g + 1) * lanes],
            xt.at[g * stack : (g + 1) * stack],
            sem_in.at[g],
        )
        for g in range(groups)
    ]
    for copy in state:
        copy.start()
    peers, begin, finish, drain = gather_plan(gath, sends, receives)
    barrier = pltpu.get_barrier_semaphore()
    for place in peers:
        pl.semaphore_signal(barrier, inc=1, device_id=place, device_id_type=MESH)

    local = cell_ref[...] - order_s[me] * columns
    here = jnp.logical_and(local >= 0, local < columns)
    ahead = here.astype(jnp.int32)
    total = ahead
    along = lax.broadcasted_iota(jnp.int32, (batches, obs), 1)
    step = 1
    while step < obs:
        ahead = ahead + jnp.where(along >= step, pltpu.roll(ahead, step, axis=1), 0)
        total = total + pltpu.roll(total, step, axis=1)
        step *= 2
    code = stack_ref[...] * columns + local
    slot_of = lax.broadcasted_iota(jnp.int32, (cap, obs), 0) + round_s[0] * cap + 1
    codes = jnp.zeros((cap, obs), jnp.int32)
    earlier = jnp.zeros((1, obs), jnp.int32)
    for b in range(batches):
        mine = jnp.where(here[b : b + 1], ahead[b : b + 1] + earlier, 0)
        codes = codes + jnp.where(mine == slot_of, code[b : b + 1], 0)
        earlier = earlier + total[b : b + 1]
    step = 1
    while step < obs:
        codes = codes + pltpu.roll(codes, step, axis=1)
        step *= 2
    list_v[...] = codes
    listing = pltpu.make_async_copy(list_v, list_s, sem_list)
    listing.start()

    first = (round_s[0] * cap).astype(jnp.float32)
    number = lax.broadcasted_iota(jnp.int32, (devices, obs), 0).astype(jnp.float32)
    square = (devices, devices)
    same = lax.broadcasted_iota(jnp.int32, square, 0) == lax.broadcasted_iota(jnp.int32, square, 1)
    order = jnp.sum(
        jnp.where(same, order_ref[...].astype(jnp.float32), 0.0), axis=1, keepdims=True
    )
    before = lax.broadcasted_iota(jnp.int32, (obs, obs), 0) < lax.broadcasted_iota(
        jnp.int32, (obs, obs), 1
    )
    before = before.astype(jnp.bfloat16)
    count = jnp.zeros((devices, 1), jnp.float32)
    slots = []
    for b in range(batches):
        cells = cell_ref[b : b + 1, :].astype(jnp.float32)
        tile = jnp.floor((cells + 0.5) / columns)
        holds = (order == tile).astype(jnp.float32)
        rank = count + jnp.dot(
            holds.astype(jnp.bfloat16), before, preferred_element_type=jnp.float32
        )
        count = count + jnp.sum(holds, axis=1, keepdims=True)
        rank = jnp.sum(holds * rank, axis=0, keepdims=True) - first
        holder = jnp.sum(holds * number, axis=0, keepdims=True)
        now = jnp.logical_and(rank >= 0.0, rank < cap)
        slots.append(jnp.where(now, holder * cap + rank, -1.0))
    rounds_s[0] = jnp.max(jnp.floor((count + (cap - 0.5)) / cap)).astype(jnp.int32)
    listing.wait()
    for copy in state:
        copy.wait()

    lane = lax.broadcasted_iota(jnp.int32, (members, lanes), 1)
    row8 = lax.broadcasted_iota(jnp.int32, (8, lanes), 0)
    lane8 = lax.broadcasted_iota(jnp.int32, (8, lanes), 1)

    def pick(k, carry):
        held, flags = carry
        code = list_s[k, 0]
        level = lax.div(code, columns)
        local = code - level * columns
        group = lax.div(local, lanes)
        block = xt[group * stack + level]
        moved = pltpu.roll(block, lax.rem(k - (local - group * lanes) + lanes, lanes), axis=1)
        held = jnp.where(lane == k, moved, held)
        flag = jnp.where(row8 == 0, ocean_s[local].astype(jnp.float32), 0.0)
        return held, jnp.where(lane8 == k, flag, flags)

    held, flags = lax.fori_loop(
        0,
        cap,
        pick,
        (jnp.zeros((members, lanes), jnp.float32), jnp.zeros((8, lanes), jnp.float32)),
        unroll=8,
    )
    rest = jnp.zeros((lanes - members - 8, lanes), jnp.float32)
    gath[me] = jnp.transpose(jnp.concatenate([held, flags, rest], axis=0))[0:cap, :]

    pl.semaphore_wait(barrier, len(peers))
    begin()
    at = lax.broadcasted_iota(jnp.int32, (obs, devices * cap), 1).astype(jnp.float32)
    for b in range(batches):
        place_t[b * obs : (b + 1) * obs, :] = (column_of(slots[b]) == at).astype(jnp.bfloat16)
    finish()

    got = jnp.concatenate([gath[k] for k in range(devices)], axis=0)
    high, low = split(got)
    rest = (got - high.astype(jnp.float32) - low.astype(jnp.float32)).astype(jnp.bfloat16)
    parts = jnp.dot(
        place_t[...],
        jnp.concatenate([high, low, rest], axis=1),
        preferred_element_type=jnp.float32,
    )
    placed = parts[:, 0:lanes] + parts[:, lanes : 2 * lanes] + parts[:, 2 * lanes :]
    for b in range(batches):
        flat_ref[b] = jnp.transpose(placed[b * obs : (b + 1) * obs, :])
    drain()


def split(values):
    high = values.astype(jnp.bfloat16)
    low = (values - high.astype(jnp.float32)).astype(jnp.bfloat16)
    return high, low


def triple(values, axis):
    high, low = split(values)
    return jnp.concatenate([high, low, high], axis=axis)


def product(left, right):
    high, low = split(left)
    return lax.dot_general(
        jnp.concatenate([high, high, low], axis=1),
        triple(right, 1),
        NT,
        preferred_element_type=jnp.float32,
    )


def update_kernel(
    order_s,
    ocean_ref,
    cell_ref,
    start_ref,
    span_ref,
    value_ref,
    mean_ref,
    spread_ref,
    shared_ref,
    x_hbm,
    y_hbm,
    xt,
    side_a,
    side_d,
    lhs_a,
    lhs_d,
    weight,
    held,
    sem_in,
    sem_out,
):
    stack, members, columns = xt.shape
    batches, obs = cell_ref.shape

    def incoming(v):
        return pltpu.make_async_copy(x_hbm.at[v], xt.at[v], sem_in.at[v])

    def outgoing(v):
        return pltpu.make_async_copy(xt.at[v], y_hbm.at[v], sem_out.at[v])

    def begin(v, c):
        incoming(v).start()
        return c

    lax.fori_loop(0, stack, begin, 0)

    base = (order_s[device_number()] * columns).astype(jnp.float32)
    places = base + lax.broadcasted_iota(jnp.int32, (1, columns), 1).astype(jnp.float32)
    ocean = ocean_ref[...].astype(jnp.float32)
    cells = cell_ref[...].astype(jnp.float32)
    starts = start_ref[...].astype(jnp.float32)
    ends = (start_ref[...] + span_ref[...]).astype(jnp.float32)
    priors = [shared_ref[b, 0:members, :] for b in range(batches)]
    flags = [shared_ref[b, members : members + 1, :] for b in range(batches)]
    scale = 1.0 / (members - 1.0)
    meets = jnp.logical_and(starts < base + columns, ends > base).astype(jnp.float32)
    before = lax.broadcasted_iota(jnp.int32, (obs, obs), 0) < lax.broadcasted_iota(
        jnp.int32, (obs, obs), 1
    )
    ranks = jnp.dot(
        jnp.concatenate([meets, jnp.zeros((16 - batches, obs), jnp.float32)], axis=0).astype(
            jnp.bfloat16
        ),
        before.astype(jnp.bfloat16),
        preferred_element_type=jnp.float32,
    )
    most = jnp.max(jnp.sum(meets, axis=1)).astype(jnp.int32)

    for b in range(batches):
        now = priors[b]
        centre = jnp.mean(now, axis=0, keepdims=True)
        anomalies = now - centre
        innovation = jnp.broadcast_to(value_ref[b : b + 1, :] - centre, (16, obs))
        mean_weights = product(innovation, mean_ref[b])[0:1]
        delta = mean_weights - product(anomalies, spread_ref[b])
        scaled = anomalies * scale
        high = scaled.astype(jnp.bfloat16).astype(jnp.float32)
        stacked = jnp.concatenate([high, high, scaled - high], axis=0)
        side_a[b] = stacked.astype(jnp.bfloat16)
        d_high, d_low = split(delta)
        side_d[b, 0] = d_high
        side_d[b, 1] = d_low
        if b + 1 < batches:
            start_of = jnp.transpose(jnp.broadcast_to(starts[b : b + 1], (128, obs)))[:, 0:1]
            end_of = jnp.transpose(jnp.broadcast_to(ends[b : b + 1], (128, obs)))[:, 0:1]
            later = jnp.concatenate(priors[b + 1 :], axis=1)
            cell_row = jnp.concatenate([cells[a : a + 1] for a in range(b + 1, batches)], axis=1)
            flag_row = jnp.concatenate(flags[b + 1 :], axis=1)
            inside = jnp.where(
                jnp.logical_and(cell_row >= start_of, cell_row < end_of), flag_row, 0.0
            )
            gain = inside * jnp.dot(
                jnp.transpose(stacked).astype(jnp.bfloat16),
                triple(later, 0),
                preferred_element_type=jnp.float32,
            )
            later = later + jnp.dot(
                jnp.concatenate([d_high, d_high, d_low], axis=1),
                triple(gain, 0),
                preferred_element_type=jnp.float32,
            )
            for a in range(b + 1, batches):
                priors[a] = later[:, (a - b - 1) * obs : (a - b) * obs]

    def sweep_with(kept):
        together = most_levels(stack, held.shape[0] if kept == min(SIZES) else 5)
        slot = lax.broadcasted_iota(jnp.int32, (kept, obs), 0).astype(jnp.float32)
        before_d = None
        for b in range(batches):
            chosen = jnp.logical_and(slot == ranks[b : b + 1], meets[b : b + 1] > 0.0)
            start_of = jnp.sum(jnp.where(chosen, starts[b : b + 1], 0.0), axis=1, keepdims=True)
            end_of = jnp.sum(jnp.where(chosen, ends[b : b + 1], 0.0), axis=1, keepdims=True)
            weight[b, 0:kept] = jnp.where(
                jnp.logical_and(places >= start_of, places < end_of), ocean, 0.0
            )
            pick = chosen.astype(jnp.bfloat16)
            second = b % 2
            rows = slice(second * kept, second * kept + kept)
            lhs_a[b // 2, rows] = lax.dot_general(
                pick, side_a[b], NT, preferred_element_type=jnp.float32
            ).astype(jnp.bfloat16)
            highs = lax.dot_general(side_d[b, 0], pick, NT, preferred_element_type=jnp.float32)
            lows = lax.dot_general(side_d[b, 1], pick, NT, preferred_element_type=jnp.float32)
            parts = jnp.concatenate([highs, highs, lows], axis=1).astype(jnp.bfloat16)
            lhs_d[b, 0:members, 0 : 3 * kept] = parts
            if second:
                cross = jnp.dot(
                    lhs_a[b // 2, rows],
                    before_d,
                    preferred_element_type=jnp.float32,
                )
                c_high, c_low = split(cross)
                lhs_d[b - 1, members : members + kept, 0 : 3 * kept] = jnp.concatenate([c_high, c_high, c_low], axis=1)
            else:
                before_d = jnp.concatenate([highs, lows, highs], axis=0).astype(jnp.bfloat16)

        def sweep(number, c):
            levels = [number * together + k for k in range(together)]
            for v in levels:
                incoming(v).wait()
            values = [xt[v] for v in levels]
            for b in range(0, batches, 2):
                both = []
                for k in range(together):
                    both.append(
                        jnp.dot(
                            lhs_a[b // 2, 0 : 2 * kept],
                            triple(values[k], 0),
                            preferred_element_type=jnp.float32,
                        )
                    )
                for k in range(together):
                    held[k, 0:kept] = both[k][kept:]
                moved = []
                for k in range(together):
                    gain = triple(weight[b, 0:kept] * both[k][0:kept], 0)
                    moved.append(
                        jnp.dot(
                            lhs_d[b, 0 : kept + members, 0 : 3 * kept],
                            gain,
                            preferred_element_type=jnp.float32,
                        )
                    )
                for k in range(together):
                    xt[levels[k]] = values[k] + moved[k][0:members]
                for k in range(together):
                    gain = weight[b + 1, 0:kept] * (held[k, 0:kept] + moved[k][members:])
                    values[k] = (
                        xt[levels[k]]
                        + jnp.dot(
                            lhs_d[b + 1, 0:members, 0 : 3 * kept],
                            triple(gain, 0),
                            preferred_element_type=jnp.float32,
                        )
                    )
            for k in range(together):
                xt[levels[k]] = values[k]
            for v in levels:
                outgoing(v).start()
            return c

        lax.fori_loop(0, stack // together, sweep, 0)

    sizes = [kept for kept in SIZES if kept < obs] + [obs]
    for low, kept in zip([-1] + sizes[:-1], sizes):
        pl.when(jnp.logical_and(most > low, most <= kept))(functools.partial(sweep_with, kept))

    def end(v, c):
        outgoing(v).wait()
        return c

    lax.fori_loop(0, stack, end, 0)


def per_device(
    prior,
    ocean_mask,
    tile_order,
    obs_cell,
    obs_stack,
    obs_values,
    window_start,
    window_span,
    gain_mean,
    gain_spread,
):
    members, stack, columns = prior.shape
    batches, obs = obs_cell.shape
    devices = tile_order.shape[0]
    mean = -(-batches * obs // devices)
    cap = min(round_up(mean + 4 * math.isqrt(mean), 8), 128)
    smem = pl.BlockSpec(memory_space=pltpu.SMEM)
    vmem = pl.BlockSpec(memory_space=pltpu.VMEM)
    hbm = pl.BlockSpec(memory_space=pl.ANY)

    levels = jnp.transpose(prior, (1, 0, 2))

    def share(number):
        return pl.pallas_call(
            share_kernel,
            out_shape=(
                jax.ShapeDtypeStruct((batches, 128, obs), jnp.float32),
                jax.ShapeDtypeStruct((1,), jnp.int32),
            ),
            in_specs=[smem, smem, smem, vmem, vmem, vmem, hbm],
            out_specs=(vmem, smem),
            scratch_shapes=[
                pltpu.VMEM((columns // 128 * stack, members, 128), jnp.float32),
                pltpu.VMEM((cap, obs), jnp.int32),
                pltpu.SMEM((cap, obs), jnp.int32),
                pltpu.VMEM((devices, cap, 128), jnp.float32),
                pltpu.VMEM((batches * obs, devices * cap), jnp.bfloat16),
                pltpu.SemaphoreType.DMA((columns // 128,)),
                pltpu.SemaphoreType.DMA,
                pltpu.SemaphoreType.DMA((devices,)),
                pltpu.SemaphoreType.DMA((devices,)),
            ],
            compiler_params=pltpu.CompilerParams(collective_id=0, has_side_effects=True),
            name="share",
        )(number, ocean_mask, tile_order, tile_order.reshape(1, devices), obs_cell, obs_stack, levels)

    shared, rounds = share(jnp.zeros((1,), jnp.int32))
    _, shared = lax.while_loop(
        lambda carry: carry[0] < rounds[0],
        lambda carry: (carry[0] + 1, carry[1] + share(carry[0].reshape(1))[0]),
        (jnp.int32(1), shared),
    )

    updated = pl.pallas_call(
        update_kernel,
        out_shape=jax.ShapeDtypeStruct(levels.shape, levels.dtype),
        in_specs=[smem] + [vmem] * 8 + [hbm],
        out_specs=hbm,
        scratch_shapes=[
            pltpu.VMEM((stack, members, columns), jnp.float32),
            pltpu.VMEM((batches, 3 * members, obs), jnp.bfloat16),
            pltpu.VMEM((batches, 2, members, obs), jnp.bfloat16),
            pltpu.VMEM((batches // 2, 2 * obs, 3 * members), jnp.bfloat16),
            pltpu.VMEM((batches, members + obs, 3 * obs), jnp.bfloat16),
            pltpu.VMEM((batches, obs, columns), jnp.float32),
            pltpu.VMEM((most_levels(stack, 10), obs, columns), jnp.float32),
            pltpu.SemaphoreType.DMA((stack,)),
            pltpu.SemaphoreType.DMA((stack,)),
        ],
        name="update",
    )(
        tile_order,
        ocean_mask.reshape(1, columns),
        obs_cell,
        window_start,
        window_span,
        obs_values,
        gain_mean,
        gain_spread,
        shared,
        levels,
    )
    return jnp.transpose(updated, (1, 0, 2))


def solution(mesh):
    in_specs = (P(None, None, ("row", "col")), P(("row", "col"))) + (P(),) * 8
    return jax.shard_map(
        per_device,
        mesh=mesh,
        in_specs=in_specs,
        out_specs=P(None, None, ("row", "col")),
        check_vma=False,
    )
```

```python
import functools
import math

import jax
import jax.numpy as jnp
from jax import lax
from jax.experimental import pallas as pl
from jax.experimental.pallas import tpu as pltpu
from jax.sharding import PartitionSpec as P

MESH = pl.DeviceIdType.MESH
NT = (((1,), (1,)), ((), ()))
SIZES = (48, 80)


def device_number():
    return lax.axis_index("row") * lax.axis_size("col") + lax.axis_index("col")


def round_up(number, step):
    return (number + step - 1) // step * step


def mate(index, step, size):
    if size & (size - 1):
        return lax.rem(index + step, size)
    bit = 1
    while bit <= step:
        if step & bit:
            index = index + bit - 2 * bit * (index // bit % 2)
        bit *= 2
    return index


def most_levels(stack, limit):
    return max(k for k in range(1, limit + 1) if stack % k == 0)


def gather_plan(gath, sends, receives):
    rows, cols = lax.axis_size("row"), lax.axis_size("col")
    plane = cols // 2
    row, col = lax.axis_index("row"), lax.axis_index("col")
    core, chip = lax.rem(col, 2), col // 2
    other = (row, chip * 2 + 1 - core)
    steps = [(a, b) for a in range(rows) for b in range(plane) if a or b]
    steps.sort(key=lambda step: step[0] + step[1].bit_count())

    def place(step):
        return (mate(row, step[0], rows), mate(chip, step[1], plane) * 2 + core)

    def slot(step, twin):
        return (
            mate(row, step[0], rows) * cols
            + mate(chip, step[1], plane) * 2
            + (1 - core if twin else core)
        )

    started = []

    def send(number, to):
        copy = pltpu.make_async_remote_copy(
            src_ref=gath.at[number],
            dst_ref=gath.at[number],
            send_sem=sends.at[len(started)],
            recv_sem=receives.at[number],
            device_id=to,
            device_id_type=MESH,
        )
        copy.start()
        started.append(copy)

    def arrive(number):
        pltpu.make_async_remote_copy(
            src_ref=gath.at[number],
            dst_ref=gath.at[number],
            send_sem=sends.at[0],
            recv_sem=receives.at[number],
            device_id=other,
            device_id_type=MESH,
        ).wait_recv()

    def begin():
        mine = slot((0, 0), False)
        for step in reversed(steps):
            send(mine, place(step))
        send(mine, other)

    def finish():
        for step in steps:
            number = slot(step, False)
            arrive(number)
            send(number, other)
        for step in [(0, 0)] + steps:
            arrive(slot(step, True))

    def drain():
        for copy in started:
            copy.wait_send()

    return [place(step) for step in steps] + [other], begin, finish, drain


def share_kernel(
    round_s,
    ocean_s,
    order_s,
    order_ref,
    cell_ref,
    stack_ref,
    x_hbm,
    flat_ref,
    rounds_s,
    xt,
    list_v,
    list_s,
    gath,
    one_hot,
    sem_in,
    sem_list,
    sends,
    receives,
):
    stack, members, columns = x_hbm.shape
    batches, obs = cell_ref.shape
    devices, piece, lanes = gath.shape
    cap = one_hot.shape[0] // devices
    groups = columns // lanes
    parts = lanes // cap
    me = device_number()
    state = [
        pltpu.make_async_copy(
            x_hbm.at[:, :, g * lanes : (g + 1) * lanes],
            xt.at[g * stack : (g + 1) * stack],
            sem_in.at[g],
        )
        for g in range(groups)
    ]
    for copy in state:
        copy.start()
    peers, begin, finish, drain = gather_plan(gath, sends, receives)
    barrier = pltpu.get_barrier_semaphore()
    for place in peers:
        pl.semaphore_signal(barrier, inc=1, device_id=place, device_id_type=MESH)

    local = cell_ref[...] - order_s[me] * columns
    here = jnp.logical_and(local >= 0, local < columns)
    ahead = here.astype(jnp.int32)
    total = ahead
    along = lax.broadcasted_iota(jnp.int32, (batches, obs), 1)
    step = 1
    while step < obs:
        ahead = ahead + jnp.where(along >= step, pltpu.roll(ahead, step, axis=1), 0)
        total = total + pltpu.roll(total, step, axis=1)
        step *= 2
    code = stack_ref[...] * columns + local
    slot_of = lax.broadcasted_iota(jnp.int32, (cap, obs), 0) + round_s[0] * cap + 1
    codes = jnp.zeros((cap, obs), jnp.int32)
    earlier = jnp.zeros((1, obs), jnp.int32)
    for b in range(batches):
        mine = jnp.where(here[b : b + 1], ahead[b : b + 1] + earlier, 0)
        codes = codes + jnp.where(mine == slot_of, code[b : b + 1], 0)
        earlier = earlier + total[b : b + 1]
    step = 1
    while step < obs:
        codes = codes + pltpu.roll(codes, step, axis=1)
        step *= 2
    diagonal = lax.broadcasted_iota(jnp.int32, (cap, obs), 0) == lax.broadcasted_iota(
        jnp.int32, (cap, obs), 1
    )
    list_v[...] = jnp.broadcast_to(
        jnp.sum(jnp.where(diagonal, codes, 0), axis=0, keepdims=True), list_v.shape
    )
    listing = pltpu.make_async_copy(list_v, list_s, sem_list)
    listing.start()

    first = (round_s[0] * cap).astype(jnp.float32)
    number = lax.broadcasted_iota(jnp.int32, (devices, obs), 0).astype(jnp.float32)
    square = (devices, devices)
    same = lax.broadcasted_iota(jnp.int32, square, 0) == lax.broadcasted_iota(jnp.int32, square, 1)
    order = jnp.sum(
        jnp.where(same, order_ref[...].astype(jnp.float32), 0.0), axis=1, keepdims=True
    )
    before = lax.broadcasted_iota(jnp.int32, (obs, obs), 0) < lax.broadcasted_iota(
        jnp.int32, (obs, obs), 1
    )
    before = before.astype(jnp.bfloat16)
    count = jnp.zeros((devices, 1), jnp.float32)
    slots = []
    for b in range(batches):
        cells = cell_ref[b : b + 1, :].astype(jnp.float32)
        tile = jnp.floor((cells + 0.5) / columns)
        holds = (order == tile).astype(jnp.float32)
        rank = count + jnp.dot(
            holds.astype(jnp.bfloat16), before, preferred_element_type=jnp.float32
        )
        count = count + jnp.sum(holds, axis=1, keepdims=True)
        rank = jnp.sum(holds * rank, axis=0, keepdims=True) - first
        holder = jnp.sum(holds * number, axis=0, keepdims=True)
        now = jnp.logical_and(rank >= 0.0, rank < cap)
        slots.append(jnp.where(now, holder * cap + rank, -1.0))
    rounds_s[0] = jnp.max(jnp.floor((count + (cap - 0.5)) / cap)).astype(jnp.int32)
    listing.wait()
    for copy in state:
        copy.wait()

    lane = lax.broadcasted_iota(jnp.int32, (members, lanes), 1)
    row8 = lax.broadcasted_iota(jnp.int32, (8, lanes), 0)
    lane8 = lax.broadcasted_iota(jnp.int32, (8, lanes), 1)

    def pick(k, carry):
        held, flags = carry
        code = list_s[0, k]
        level = lax.div(code, columns)
        local = code - level * columns
        group = lax.div(local, lanes)
        block = xt[group * stack + level]
        moved = pltpu.roll(block, lax.rem(k - (local - group * lanes) + lanes, lanes), axis=1)
        held = jnp.where(lane == k, moved, held)
        flag = jnp.where(row8 == 0, ocean_s[local].astype(jnp.float32), 0.0)
        return held, jnp.where(lane8 == k, flag, flags)

    held, flags = lax.fori_loop(
        0,
        cap,
        pick,
        (jnp.zeros((members, lanes), jnp.float32), jnp.zeros((8, lanes), jnp.float32)),
        unroll=8,
    )
    rest = jnp.zeros((parts * piece - members - 8, lanes), jnp.float32)
    held = jnp.concatenate([held, flags, rest], axis=0)
    part_of = lax.broadcasted_iota(jnp.int32, (piece, lanes), 1) // cap
    packed = held[0:piece]
    for g in range(1, parts):
        moved = pltpu.roll(held[g * piece : (g + 1) * piece], g * cap, axis=1)
        packed = jnp.where(part_of == g, moved, packed)
    gath[me] = packed

    pl.semaphore_wait(barrier, len(peers))
    begin()
    at = lax.broadcasted_iota(jnp.int32, (devices * cap, obs), 0).astype(jnp.float32)
    for b in range(batches):
        one_hot[:, b * obs : (b + 1) * obs] = (slots[b] == at).astype(jnp.bfloat16)
    finish()

    unpacked = []
    for g in range(parts):
        tiles = []
        for first_device in range(0, devices, parts):
            tile = None
            for q in range(parts):
                moved = gath[first_device + q]
                if q != g:
                    moved = pltpu.roll(moved, (q - g) % parts * cap, axis=1)
                tile = moved if q == 0 else jnp.where(part_of == q, moved, tile)
            tiles.append(tile)
        unpacked.append(jnp.concatenate(tiles, axis=1))
    high, low = split(jnp.concatenate(unpacked, axis=0))
    placed = jnp.dot(
        jnp.concatenate([high, low], axis=0), one_hot[...], preferred_element_type=jnp.float32
    )
    height = parts * piece
    placed = placed[0:height] + placed[height:]
    for b in range(batches):
        flat_ref[b] = placed[:, b * obs : (b + 1) * obs]
    drain()


def split(values):
    high = values.astype(jnp.bfloat16)
    low = (values - high.astype(jnp.float32)).astype(jnp.bfloat16)
    return high, low


def triple(values, axis):
    high, low = split(values)
    return jnp.concatenate([high, low, high], axis=axis)


def product(left, right):
    high, low = split(left)
    return lax.dot_general(
        jnp.concatenate([high, high, low], axis=1),
        triple(right, 1),
        NT,
        preferred_element_type=jnp.float32,
    )


def update_kernel(
    order_s,
    ocean_ref,
    cell_ref,
    start_ref,
    span_ref,
    value_ref,
    mean_ref,
    spread_ref,
    shared_ref,
    x_hbm,
    y_hbm,
    xt,
    side_a,
    side_d,
    lhs_a,
    lhs_d,
    weight,
    held,
    sem_in,
    sem_out,
):
    stack, members, columns = xt.shape
    batches, obs = cell_ref.shape

    def incoming(v):
        return pltpu.make_async_copy(x_hbm.at[v], xt.at[v], sem_in.at[v])

    def outgoing(v):
        return pltpu.make_async_copy(xt.at[v], y_hbm.at[v], sem_out.at[v])

    def begin(v, c):
        incoming(v).start()
        return c

    lax.fori_loop(0, stack, begin, 0)

    base = (order_s[device_number()] * columns).astype(jnp.float32)
    places = base + lax.broadcasted_iota(jnp.int32, (1, columns), 1).astype(jnp.float32)
    ocean = ocean_ref[...].astype(jnp.float32)
    cells = cell_ref[...].astype(jnp.float32)
    starts = start_ref[...].astype(jnp.float32)
    ends = (start_ref[...] + span_ref[...]).astype(jnp.float32)
    priors = [shared_ref[b, 0:members, :] for b in range(batches)]
    flags = [shared_ref[b, members : members + 1, :] for b in range(batches)]
    scale = 1.0 / (members - 1.0)
    meets = jnp.logical_and(starts < base + columns, ends > base).astype(jnp.float32)
    before = lax.broadcasted_iota(jnp.int32, (obs, obs), 0) < lax.broadcasted_iota(
        jnp.int32, (obs, obs), 1
    )
    ranks = jnp.dot(
        jnp.concatenate([meets, jnp.zeros((16 - batches, obs), jnp.float32)], axis=0).astype(
            jnp.bfloat16
        ),
        before.astype(jnp.bfloat16),
        preferred_element_type=jnp.float32,
    )
    most = jnp.max(jnp.sum(meets, axis=1)).astype(jnp.int32)

    for b in range(batches):
        now = priors[b]
        centre = jnp.mean(now, axis=0, keepdims=True)
        anomalies = now - centre
        innovation = jnp.broadcast_to(value_ref[b : b + 1, :] - centre, (16, obs))
        mean_weights = product(innovation, mean_ref[b])[0:1]
        delta = mean_weights - product(anomalies, spread_ref[b])
        scaled = anomalies * scale
        high = scaled.astype(jnp.bfloat16).astype(jnp.float32)
        stacked = jnp.concatenate([high, high, scaled - high], axis=0)
        side_a[b] = stacked.astype(jnp.bfloat16)
        d_high, d_low = split(delta)
        side_d[b, 0] = d_high
        side_d[b, 1] = d_low
        if b + 1 < batches:
            start_of = jnp.transpose(jnp.broadcast_to(starts[b : b + 1], (128, obs)))[:, 0:1]
            end_of = jnp.transpose(jnp.broadcast_to(ends[b : b + 1], (128, obs)))[:, 0:1]
            later = jnp.concatenate(priors[b + 1 :], axis=1)
            cell_row = jnp.concatenate([cells[a : a + 1] for a in range(b + 1, batches)], axis=1)
            flag_row = jnp.concatenate(flags[b + 1 :], axis=1)
            inside = jnp.where(
                jnp.logical_and(cell_row >= start_of, cell_row < end_of), flag_row, 0.0
            )
            gain = inside * jnp.dot(
                jnp.transpose(stacked).astype(jnp.bfloat16),
                triple(later, 0),
                preferred_element_type=jnp.float32,
            )
            later = later + jnp.dot(
                jnp.concatenate([d_high, d_high, d_low], axis=1),
                triple(gain, 0),
                preferred_element_type=jnp.float32,
            )
            for a in range(b + 1, batches):
                priors[a] = later[:, (a - b - 1) * obs : (a - b) * obs]

    def sweep_with(kept):
        together = most_levels(stack, held.shape[0] if kept == min(SIZES) else 5)
        slot = lax.broadcasted_iota(jnp.int32, (kept, obs), 0).astype(jnp.float32)
        before_d = None
        for b in range(batches):
            chosen = jnp.logical_and(slot == ranks[b : b + 1], meets[b : b + 1] > 0.0)
            start_of = jnp.sum(jnp.where(chosen, starts[b : b + 1], 0.0), axis=1, keepdims=True)
            end_of = jnp.sum(jnp.where(chosen, ends[b : b + 1], 0.0), axis=1, keepdims=True)
            weight[b, 0:kept] = jnp.where(
                jnp.logical_and(places >= start_of, places < end_of), ocean, 0.0
            )
            pick = chosen.astype(jnp.bfloat16)
            second = b % 2
            rows = slice(second * kept, second * kept + kept)
            lhs_a[b // 2, rows] = lax.dot_general(
                pick, side_a[b], NT, preferred_element_type=jnp.float32
            ).astype(jnp.bfloat16)
            highs = lax.dot_general(side_d[b, 0], pick, NT, preferred_element_type=jnp.float32)
            lows = lax.dot_general(side_d[b, 1], pick, NT, preferred_element_type=jnp.float32)
            parts = jnp.concatenate([highs, highs, lows], axis=1).astype(jnp.bfloat16)
            lhs_d[b, 0:members, 0 : 3 * kept] = parts
            if second:
                cross = jnp.dot(
                    lhs_a[b // 2, rows],
                    before_d,
                    preferred_element_type=jnp.float32,
                )
                c_high, c_low = split(cross)
                lhs_d[b - 1, members : members + kept, 0 : 3 * kept] = jnp.concatenate([c_high, c_high, c_low], axis=1)
            else:
                before_d = jnp.concatenate([highs, lows, highs], axis=0).astype(jnp.bfloat16)

        def sweep(number, c):
            levels = [number * together + k for k in range(together)]
            for v in levels:
                incoming(v).wait()
            values = [xt[v] for v in levels]
            for b in range(0, batches, 2):
                both = []
                for k in range(together):
                    both.append(
                        jnp.dot(
                            lhs_a[b // 2, 0 : 2 * kept],
                            triple(values[k], 0),
                            preferred_element_type=jnp.float32,
                        )
                    )
                for k in range(together):
                    held[k, 0:kept] = both[k][kept:]
                moved = []
                for k in range(together):
                    gain = triple(weight[b, 0:kept] * both[k][0:kept], 0)
                    moved.append(
                        jnp.dot(
                            lhs_d[b, 0 : kept + members, 0 : 3 * kept],
                            gain,
                            preferred_element_type=jnp.float32,
                        )
                    )
                for k in range(together):
                    xt[levels[k]] = values[k] + moved[k][0:members]
                for k in range(together):
                    gain = weight[b + 1, 0:kept] * (held[k, 0:kept] + moved[k][members:])
                    values[k] = (
                        xt[levels[k]]
                        + jnp.dot(
                            lhs_d[b + 1, 0:members, 0 : 3 * kept],
                            triple(gain, 0),
                            preferred_element_type=jnp.float32,
                        )
                    )
            for k in range(together):
                xt[levels[k]] = values[k]
            for v in levels:
                outgoing(v).start()
            return c

        lax.fori_loop(0, stack // together, sweep, 0)

    sizes = [kept for kept in SIZES if kept < obs] + [obs]
    for low, kept in zip([-1] + sizes[:-1], sizes):
        pl.when(jnp.logical_and(most > low, most <= kept))(functools.partial(sweep_with, kept))

    def end(v, c):
        outgoing(v).wait()
        return c

    lax.fori_loop(0, stack, end, 0)


def per_device(
    prior,
    ocean_mask,
    tile_order,
    obs_cell,
    obs_stack,
    obs_values,
    window_start,
    window_span,
    gain_mean,
    gain_spread,
):
    members, stack, columns = prior.shape
    batches, obs = obs_cell.shape
    devices = tile_order.shape[0]
    mean = -(-batches * obs // devices)
    cap = 8
    while cap < min(mean + 4 * math.isqrt(mean), 128):
        cap *= 2
    parts = 128 // cap
    piece = round_up(-(-(members + 8) // parts), 8)
    smem = pl.BlockSpec(memory_space=pltpu.SMEM)
    vmem = pl.BlockSpec(memory_space=pltpu.VMEM)
    hbm = pl.BlockSpec(memory_space=pl.ANY)

    levels = jnp.transpose(prior, (1, 0, 2))

    def share(number):
        return pl.pallas_call(
            share_kernel,
            out_shape=(
                jax.ShapeDtypeStruct((batches, parts * piece, obs), jnp.float32),
                jax.ShapeDtypeStruct((1,), jnp.int32),
            ),
            in_specs=[smem, smem, smem, vmem, vmem, vmem, hbm],
            out_specs=(vmem, smem),
            scratch_shapes=[
                pltpu.VMEM((columns // 128 * stack, members, 128), jnp.float32),
                pltpu.VMEM((1, obs), jnp.int32),
                pltpu.SMEM((1, obs), jnp.int32),
                pltpu.VMEM((devices, piece, 128), jnp.float32),
                pltpu.VMEM((devices * cap, batches * obs), jnp.bfloat16),
                pltpu.SemaphoreType.DMA((columns // 128,)),
                pltpu.SemaphoreType.DMA,
                pltpu.SemaphoreType.DMA((devices,)),
                pltpu.SemaphoreType.DMA((devices,)),
            ],
            compiler_params=pltpu.CompilerParams(collective_id=0, has_side_effects=True),
            name="share",
        )(number, ocean_mask, tile_order, tile_order.reshape(1, devices), obs_cell, obs_stack, levels)

    shared, rounds = share(jnp.zeros((1,), jnp.int32))
    _, shared = lax.while_loop(
        lambda carry: carry[0] < rounds[0],
        lambda carry: (carry[0] + 1, carry[1] + share(carry[0].reshape(1))[0]),
        (jnp.int32(1), shared),
    )

    updated = pl.pallas_call(
        update_kernel,
        out_shape=jax.ShapeDtypeStruct(levels.shape, levels.dtype),
        in_specs=[smem] + [vmem] * 8 + [hbm],
        out_specs=hbm,
        scratch_shapes=[
            pltpu.VMEM((stack, members, columns), jnp.float32),
            pltpu.VMEM((batches, 3 * members, obs), jnp.bfloat16),
            pltpu.VMEM((batches, 2, members, obs), jnp.bfloat16),
            pltpu.VMEM((batches // 2, 2 * obs, 3 * members), jnp.bfloat16),
            pltpu.VMEM((batches, members + obs, 3 * obs), jnp.bfloat16),
            pltpu.VMEM((batches, obs, columns), jnp.float32),
            pltpu.VMEM((most_levels(stack, 10), obs, columns), jnp.float32),
            pltpu.SemaphoreType.DMA((stack,)),
            pltpu.SemaphoreType.DMA((stack,)),
        ],
        name="update",
    )(
        tile_order,
        ocean_mask.reshape(1, columns),
        obs_cell,
        window_start,
        window_span,
        obs_values,
        gain_mean,
        gain_spread,
        shared,
        levels,
    )
    return jnp.transpose(updated, (1, 0, 2))


def solution(mesh):
    in_specs = (P(None, None, ("row", "col")), P(("row", "col"))) + (P(),) * 8
    return jax.shard_map(
        per_device,
        mesh=mesh,
        in_specs=in_specs,
        out_specs=P(None, None, ("row", "col")),
        check_vma=False,
    )
```

```python
import functools
import math

import jax
import jax.numpy as jnp
from jax import lax
from jax.experimental import pallas as pl
from jax.experimental.pallas import tpu as pltpu
from jax.sharding import PartitionSpec as P

MESH = pl.DeviceIdType.MESH
NT = (((1,), (1,)), ((), ()))
SIZES = (48, 80)


def device_number():
    return lax.axis_index("row") * lax.axis_size("col") + lax.axis_index("col")


def round_up(number, step):
    return (number + step - 1) // step * step


def mate(index, step, size):
    if size & (size - 1):
        return lax.rem(index + step, size)
    bit = 1
    while bit <= step:
        if step & bit:
            index = index + bit - 2 * bit * (index // bit % 2)
        bit *= 2
    return index


def most_levels(stack, limit):
    return max(k for k in range(1, limit + 1) if stack % k == 0)


def gather_plan(gath, used, sends, receives):
    rows, cols = lax.axis_size("row"), lax.axis_size("col")
    plane = cols // 2
    row, col = lax.axis_index("row"), lax.axis_index("col")
    core, chip = lax.rem(col, 2), col // 2
    other = (row, chip * 2 + 1 - core)
    steps = [(a, b) for a in range(rows) for b in range(plane) if a or b]
    steps.sort(key=lambda step: step[0] + step[1].bit_count())
    ranked = [sorted(range(rows), key=lambda other: abs(other - here)) for here in range(rows)]

    def near_row(step):
        index = ranked[0][step]
        for here in range(1, rows):
            index = jnp.where(row == here, ranked[here][step], index)
        return index

    order = [near_row(step) for step in range(rows)]

    def place(step, twin=False):
        side = 1 - core if twin else core
        return (order[step[0]], mate(chip, step[1], plane) * 2 + side)

    def slot(step, twin):
        return order[step[0]] * cols + mate(chip, step[1], plane) * 2 + (1 - core if twin else core)

    started = []

    def send(number, to):
        copy = pltpu.make_async_remote_copy(
            src_ref=gath.at[number, 0:used],
            dst_ref=gath.at[number, 0:used],
            send_sem=sends.at[len(started)],
            recv_sem=receives.at[number],
            device_id=to,
            device_id_type=MESH,
        )
        copy.start()
        started.append(copy)

    def arrive(number):
        pltpu.make_async_remote_copy(
            src_ref=gath.at[number, 0:used],
            dst_ref=gath.at[number, 0:used],
            send_sem=sends.at[0],
            recv_sem=receives.at[number],
            device_id=other,
            device_id_type=MESH,
        ).wait_recv()

    def begin():
        mine = slot((0, 0), False)
        for step in reversed(steps):
            send(mine, place(step))
            if not step[0]:
                send(mine, place(step, True))
        send(mine, other)

    def relay():
        for step in steps:
            number = slot(step, False)
            arrive(number)
            if step[0]:
                send(number, other)

    def collect(row_step):
        for step in range(plane):
            arrive(slot((row_step, step), True))
        return order[row_step]

    def drain():
        for copy in started:
            copy.wait_send()

    twins = [place(step, True) for step in steps if not step[0]]
    return [place(step) for step in steps] + twins + [other], begin, relay, collect, drain


def share_kernel(
    round_in,
    ocean_in,
    order_in,
    order_row,
    cell_in,
    stack_in,
    x_hbm,
    flat_ref,
    rounds_s,
    round_s,
    ocean_s,
    order_s,
    order_ref,
    cell_ref,
    stack_ref,
    xt,
    list_v,
    list_s,
    gath,
    one_hot,
    total_ref,
    sem_small,
    sem_in,
    sem_list,
    sends,
    receives,
):
    stack, members, columns = x_hbm.shape
    batches, obs = cell_ref.shape
    devices, piece, lanes = gath.shape
    cap = one_hot.shape[0] // devices
    groups = columns // lanes
    parts = lanes // cap
    used = -(-(members + 1) // parts)
    me = device_number()
    state = [
        pltpu.make_async_copy(
            x_hbm.at[:, :, g * lanes : (g + 1) * lanes],
            xt.at[g * stack : (g + 1) * stack],
            sem_in.at[g],
        )
        for g in range(groups)
    ]
    pairs = (
        (order_in, order_s),
        (cell_in, cell_ref),
        (stack_in, stack_ref),
        (round_in, round_s),
        (order_row, order_ref),
        (ocean_in, ocean_s),
    )
    small = [
        pltpu.make_async_copy(source, target, sem_small.at[k])
        for k, (source, target) in enumerate(pairs)
    ]
    for copy in small + state:
        copy.start()
    peers, begin, relay, collect, drain = gather_plan(gath, used, sends, receives)
    barrier = pltpu.get_barrier_semaphore()
    for place in peers:
        pl.semaphore_signal(barrier, inc=1, device_id=place, device_id_type=MESH)
    for copy in small:
        copy.wait()

    local = cell_ref[...] - order_s[me] * columns
    here = jnp.logical_and(local >= 0, local < columns)
    ahead = here.astype(jnp.int32)
    total = ahead
    along = lax.broadcasted_iota(jnp.int32, (batches, obs), 1)
    step = 1
    while step < obs:
        ahead = ahead + jnp.where(along >= step, pltpu.roll(ahead, step, axis=1), 0)
        total = total + pltpu.roll(total, step, axis=1)
        step *= 2
    code = stack_ref[...] * columns + local
    slot_of = lax.broadcasted_iota(jnp.int32, (cap, obs), 0) + round_s[0] * cap + 1
    codes = jnp.zeros((cap, obs), jnp.int32)
    earlier = jnp.zeros((1, obs), jnp.int32)
    for b in range(batches):
        mine = jnp.where(here[b : b + 1], ahead[b : b + 1] + earlier, 0)
        codes = codes + jnp.where(mine == slot_of, code[b : b + 1], 0)
        earlier = earlier + total[b : b + 1]
    step = 1
    while step < obs:
        codes = codes + pltpu.roll(codes, step, axis=1)
        step *= 2
    diagonal = lax.broadcasted_iota(jnp.int32, (cap, obs), 0) == lax.broadcasted_iota(
        jnp.int32, (cap, obs), 1
    )
    list_v[...] = jnp.broadcast_to(
        jnp.sum(jnp.where(diagonal, codes, 0), axis=0, keepdims=True), list_v.shape
    )
    listing = pltpu.make_async_copy(list_v, list_s, sem_list)
    listing.start()

    first = (round_s[0] * cap).astype(jnp.float32)
    number = lax.broadcasted_iota(jnp.int32, (devices, obs), 0).astype(jnp.float32)
    square = (devices, devices)
    same = lax.broadcasted_iota(jnp.int32, square, 0) == lax.broadcasted_iota(jnp.int32, square, 1)
    order = jnp.sum(
        jnp.where(same, order_ref[...].astype(jnp.float32), 0.0), axis=1, keepdims=True
    )
    before = lax.broadcasted_iota(jnp.int32, (obs, obs), 0) < lax.broadcasted_iota(
        jnp.int32, (obs, obs), 1
    )
    before = before.astype(jnp.bfloat16)
    count = jnp.zeros((devices, 1), jnp.float32)
    slots = []
    for b in range(batches):
        cells = cell_ref[b : b + 1, :].astype(jnp.float32)
        tile = jnp.floor((cells + 0.5) / columns)
        holds = (order == tile).astype(jnp.float32)
        rank = count + jnp.dot(
            holds.astype(jnp.bfloat16), before, preferred_element_type=jnp.float32
        )
        count = count + jnp.sum(holds, axis=1, keepdims=True)
        rank = jnp.sum(holds * rank, axis=0, keepdims=True) - first
        holder = jnp.sum(holds * number, axis=0, keepdims=True)
        now = jnp.logical_and(rank >= 0.0, rank < cap)
        slots.append(jnp.where(now, holder * cap + rank, -1.0))
    rounds_s[0] = jnp.max(jnp.floor((count + (cap - 0.5)) / cap)).astype(jnp.int32)
    listing.wait()
    for copy in state:
        copy.wait()

    lane = lax.broadcasted_iota(jnp.int32, (members, lanes), 1)
    row8 = lax.broadcasted_iota(jnp.int32, (8, lanes), 0)
    lane8 = lax.broadcasted_iota(jnp.int32, (8, lanes), 1)

    def pick(k, carry):
        held, flags = carry
        code = list_s[0, k]
        level = lax.div(code, columns)
        local = code - level * columns
        group = lax.div(local, lanes)
        block = xt[group * stack + level]
        moved = pltpu.roll(block, lax.rem(k - (local - group * lanes) + lanes, lanes), axis=1)
        held = jnp.where(lane == k, moved, held)
        flag = jnp.where(row8 == 0, ocean_s[local].astype(jnp.float32), 0.0)
        return held, jnp.where(lane8 == k, flag, flags)

    held, flags = lax.fori_loop(
        0,
        cap,
        pick,
        (jnp.zeros((members, lanes), jnp.float32), jnp.zeros((8, lanes), jnp.float32)),
        unroll=cap,
    )
    rest = jnp.zeros((parts * piece - members, lanes), jnp.float32)
    held = jnp.concatenate([held, flags, rest], axis=0)
    part_of = lax.broadcasted_iota(jnp.int32, (piece, lanes), 1) // cap
    packed = held[0:piece]
    for g in range(1, parts):
        moved = pltpu.roll(held[g * used : g * used + piece], g * cap, axis=1)
        packed = jnp.where(part_of == g, moved, packed)
    gath[me] = packed

    pl.semaphore_wait(barrier, len(peers))
    begin()
    at = lax.broadcasted_iota(jnp.int32, (devices * cap, obs), 0).astype(jnp.float32)
    for b in range(batches):
        one_hot[:, b * obs : (b + 1) * obs] = (slots[b] == at).astype(jnp.bfloat16)
    relay()

    rows = lax.axis_size("row")
    share = devices // rows
    for row_step in range(rows):
        row = collect(row_step)
        unpacked = []
        for g in range(parts):
            tiles = []
            for begin_at in range(0, share, parts):
                tile = None
                for q in range(parts):
                    moved = gath[row * share + begin_at + q]
                    if q != g:
                        moved = pltpu.roll(moved, (q - g) % parts * cap, axis=1)
                    tile = moved if q == 0 else jnp.where(part_of == q, moved, tile)
                tiles.append(tile)
            unpacked.append(jnp.concatenate(tiles, axis=1))
        high, low = split(jnp.concatenate(unpacked, axis=0))
        start = pl.multiple_of(row * (share * cap), share * cap)
        placed = jnp.dot(
            jnp.concatenate([high, low], axis=0),
            one_hot[pl.ds(start, share * cap), :],
            preferred_element_type=jnp.float32,
        )
        placed = placed[0 : parts * piece] + placed[parts * piece :]
        if row_step == 0:
            total_ref[...] = placed
        elif row_step < rows - 1:
            total_ref[...] += placed
        else:
            placed = total_ref[...] + placed
            placed = jnp.concatenate(
                [placed[g * piece : g * piece + used] for g in range(parts)], axis=0
            )
            for b in range(batches):
                flat_ref[b, 0 : parts * used] = placed[:, b * obs : (b + 1) * obs]
    drain()


def split(values):
    high = values.astype(jnp.bfloat16)
    low = (values - high.astype(jnp.float32)).astype(jnp.bfloat16)
    return high, low


def triple(values, axis):
    high, low = split(values)
    return jnp.concatenate([high, low, high], axis=axis)


def product(left, right):
    high, low = split(left)
    return lax.dot_general(
        jnp.concatenate([high, high, low], axis=1),
        triple(right, 1),
        NT,
        preferred_element_type=jnp.float32,
    )


def update_kernel(
    order_s,
    ocean_ref,
    cell_ref,
    start_ref,
    span_ref,
    value_ref,
    mean_ref,
    spread_ref,
    shared_ref,
    x_hbm,
    y_hbm,
    xt,
    side_a,
    side_d,
    lhs_a,
    lhs_d,
    weight,
    held,
    sem_in,
    sem_out,
):
    stack, members, columns = xt.shape
    batches, obs = cell_ref.shape

    def incoming(v):
        return pltpu.make_async_copy(x_hbm.at[v], xt.at[v], sem_in.at[v])

    def outgoing(v):
        return pltpu.make_async_copy(xt.at[v], y_hbm.at[v], sem_out.at[v])

    def begin(v, c):
        incoming(v).start()
        return c

    lax.fori_loop(0, stack, begin, 0)

    base = (order_s[device_number()] * columns).astype(jnp.float32)
    places = base + lax.broadcasted_iota(jnp.int32, (1, columns), 1).astype(jnp.float32)
    ocean = ocean_ref[...].astype(jnp.float32)
    cells = cell_ref[...].astype(jnp.float32)
    starts = start_ref[...].astype(jnp.float32)
    ends = (start_ref[...] + span_ref[...]).astype(jnp.float32)
    priors = [shared_ref[b, 0:members, :] for b in range(batches)]
    flags = [shared_ref[b, members : members + 1, :] for b in range(batches)]
    scale = 1.0 / (members - 1.0)
    meets = jnp.logical_and(starts < base + columns, ends > base).astype(jnp.float32)
    before = lax.broadcasted_iota(jnp.int32, (obs, obs), 0) < lax.broadcasted_iota(
        jnp.int32, (obs, obs), 1
    )
    ranks = jnp.dot(
        jnp.concatenate([meets, jnp.zeros((16 - batches, obs), jnp.float32)], axis=0).astype(
            jnp.bfloat16
        ),
        before.astype(jnp.bfloat16),
        preferred_element_type=jnp.float32,
    )
    most = jnp.max(jnp.sum(meets, axis=1)).astype(jnp.int32)

    for b in range(batches):
        now = priors[b]
        centre = jnp.mean(now, axis=0, keepdims=True)
        anomalies = now - centre
        innovation = jnp.broadcast_to(value_ref[b : b + 1, :] - centre, (16, obs))
        mean_weights = product(innovation, mean_ref[b])[0:1]
        delta = mean_weights - product(anomalies, spread_ref[b])
        scaled = anomalies * scale
        high = scaled.astype(jnp.bfloat16).astype(jnp.float32)
        stacked = jnp.concatenate([high, high, scaled - high], axis=0)
        side_a[b] = stacked.astype(jnp.bfloat16)
        d_high, d_low = split(delta)
        side_d[b, 0] = d_high
        side_d[b, 1] = d_low
        if b + 1 < batches:
            start_of = jnp.transpose(jnp.broadcast_to(starts[b : b + 1], (128, obs)))[:, 0:1]
            end_of = jnp.transpose(jnp.broadcast_to(ends[b : b + 1], (128, obs)))[:, 0:1]
            later = jnp.concatenate(priors[b + 1 :], axis=1)
            cell_row = jnp.concatenate([cells[a : a + 1] for a in range(b + 1, batches)], axis=1)
            flag_row = jnp.concatenate(flags[b + 1 :], axis=1)
            inside = jnp.where(
                jnp.logical_and(cell_row >= start_of, cell_row < end_of), flag_row, 0.0
            )
            gain = inside * jnp.dot(
                jnp.transpose(stacked).astype(jnp.bfloat16),
                triple(later, 0),
                preferred_element_type=jnp.float32,
            )
            later = later + jnp.dot(
                jnp.concatenate([d_high, d_high, d_low], axis=1),
                triple(gain, 0),
                preferred_element_type=jnp.float32,
            )
            for a in range(b + 1, batches):
                priors[a] = later[:, (a - b - 1) * obs : (a - b) * obs]

    def sweep_with(kept):
        together = most_levels(stack, held.shape[0] if kept == min(SIZES) else 5)
        slot = lax.broadcasted_iota(jnp.int32, (kept, obs), 0).astype(jnp.float32)
        before_d = None
        for b in range(batches):
            chosen = jnp.logical_and(slot == ranks[b : b + 1], meets[b : b + 1] > 0.0)
            start_of = jnp.sum(jnp.where(chosen, starts[b : b + 1], 0.0), axis=1, keepdims=True)
            end_of = jnp.sum(jnp.where(chosen, ends[b : b + 1], 0.0), axis=1, keepdims=True)
            weight[b, 0:kept] = jnp.where(
                jnp.logical_and(places >= start_of, places < end_of), ocean, 0.0
            )
            pick = chosen.astype(jnp.bfloat16)
            second = b % 2
            rows = slice(second * kept, second * kept + kept)
            lhs_a[b // 2, rows] = lax.dot_general(
                pick, side_a[b], NT, preferred_element_type=jnp.float32
            ).astype(jnp.bfloat16)
            highs = lax.dot_general(side_d[b, 0], pick, NT, preferred_element_type=jnp.float32)
            lows = lax.dot_general(side_d[b, 1], pick, NT, preferred_element_type=jnp.float32)
            parts = jnp.concatenate([highs, highs, lows], axis=1).astype(jnp.bfloat16)
            lhs_d[b, 0:members, 0 : 3 * kept] = parts
            if second:
                cross = jnp.dot(
                    lhs_a[b // 2, rows],
                    before_d,
                    preferred_element_type=jnp.float32,
                )
                c_high, c_low = split(cross)
                lhs_d[b - 1, members : members + kept, 0 : 3 * kept] = jnp.concatenate([c_high, c_high, c_low], axis=1)
            else:
                before_d = jnp.concatenate([highs, lows, highs], axis=0).astype(jnp.bfloat16)

        def sweep(number, c):
            levels = [number * together + k for k in range(together)]
            for v in levels:
                incoming(v).wait()
            values = [xt[v] for v in levels]
            for b in range(0, batches, 2):
                both = []
                for k in range(together):
                    both.append(
                        jnp.dot(
                            lhs_a[b // 2, 0 : 2 * kept],
                            triple(values[k], 0),
                            preferred_element_type=jnp.float32,
                        )
                    )
                for k in range(together):
                    held[k, 0:kept] = both[k][kept:]
                moved = []
                for k in range(together):
                    gain = triple(weight[b, 0:kept] * both[k][0:kept], 0)
                    moved.append(
                        jnp.dot(
                            lhs_d[b, 0 : kept + members, 0 : 3 * kept],
                            gain,
                            preferred_element_type=jnp.float32,
                        )
                    )
                for k in range(together):
                    xt[levels[k]] = values[k] + moved[k][0:members]
                for k in range(together):
                    gain = weight[b + 1, 0:kept] * (held[k, 0:kept] + moved[k][members:])
                    values[k] = (
                        xt[levels[k]]
                        + jnp.dot(
                            lhs_d[b + 1, 0:members, 0 : 3 * kept],
                            triple(gain, 0),
                            preferred_element_type=jnp.float32,
                        )
                    )
            for k in range(together):
                xt[levels[k]] = values[k]
            for v in levels:
                outgoing(v).start()
            return c

        lax.fori_loop(0, stack // together, sweep, 0)

    sizes = [kept for kept in SIZES if kept < obs] + [obs]
    for low, kept in zip([-1] + sizes[:-1], sizes):
        pl.when(jnp.logical_and(most > low, most <= kept))(functools.partial(sweep_with, kept))

    def end(v, c):
        outgoing(v).wait()
        return c

    lax.fori_loop(0, stack, end, 0)


def per_device(
    prior,
    ocean_mask,
    tile_order,
    obs_cell,
    obs_stack,
    obs_values,
    window_start,
    window_span,
    gain_mean,
    gain_spread,
):
    members, stack, columns = prior.shape
    batches, obs = obs_cell.shape
    devices = tile_order.shape[0]
    mean = -(-batches * obs // devices)
    cap = 8
    while cap < min(mean + 4 * math.isqrt(mean), 128):
        cap *= 2
    parts = 128 // cap
    piece = round_up(-(-(members + 1) // parts), 8)
    smem = pl.BlockSpec(memory_space=pltpu.SMEM)
    vmem = pl.BlockSpec(memory_space=pltpu.VMEM)
    hbm = pl.BlockSpec(memory_space=pl.ANY)

    levels = jnp.transpose(prior, (1, 0, 2))

    def share(number):
        return pl.pallas_call(
            share_kernel,
            out_shape=(
                jax.ShapeDtypeStruct((batches, parts * piece, obs), jnp.float32),
                jax.ShapeDtypeStruct((1,), jnp.int32),
            ),
            in_specs=[hbm] * 7,
            out_specs=(vmem, smem),
            scratch_shapes=[
                pltpu.SMEM((1,), jnp.int32),
                pltpu.SMEM((columns,), jnp.int32),
                pltpu.SMEM((devices,), jnp.int32),
                pltpu.VMEM((1, devices), jnp.int32),
                pltpu.VMEM((batches, obs), jnp.int32),
                pltpu.VMEM((batches, obs), jnp.int32),
                pltpu.VMEM((columns // 128 * stack, members, 128), jnp.float32),
                pltpu.VMEM((1, obs), jnp.int32),
                pltpu.SMEM((1, obs), jnp.int32),
                pltpu.VMEM((devices, piece, 128), jnp.float32),
                pltpu.VMEM((devices * cap, batches * obs), jnp.bfloat16),
                pltpu.VMEM((parts * piece, batches * obs), jnp.float32),
                pltpu.SemaphoreType.DMA((6,)),
                pltpu.SemaphoreType.DMA((columns // 128,)),
                pltpu.SemaphoreType.DMA,
                pltpu.SemaphoreType.DMA((devices,)),
                pltpu.SemaphoreType.DMA((devices,)),
            ],
            compiler_params=pltpu.CompilerParams(collective_id=0, has_side_effects=True),
            name="share",
        )(number, ocean_mask, tile_order, tile_order.reshape(1, devices), obs_cell, obs_stack, levels)

    shared, rounds = share(jnp.zeros((1,), jnp.int32))
    _, shared = lax.while_loop(
        lambda carry: carry[0] < rounds[0],
        lambda carry: (carry[0] + 1, carry[1] + share(carry[0].reshape(1))[0]),
        (jnp.int32(1), shared),
    )

    updated = pl.pallas_call(
        update_kernel,
        out_shape=jax.ShapeDtypeStruct(levels.shape, levels.dtype),
        in_specs=[smem] + [vmem] * 8 + [hbm],
        out_specs=hbm,
        scratch_shapes=[
            pltpu.VMEM((stack, members, columns), jnp.float32),
            pltpu.VMEM((batches, 3 * members, obs), jnp.bfloat16),
            pltpu.VMEM((batches, 2, members, obs), jnp.bfloat16),
            pltpu.VMEM((batches // 2, 2 * obs, 3 * members), jnp.bfloat16),
            pltpu.VMEM((batches, members + obs, 3 * obs), jnp.bfloat16),
            pltpu.VMEM((batches, obs, columns), jnp.float32),
            pltpu.VMEM((most_levels(stack, 10), obs, columns), jnp.float32),
            pltpu.SemaphoreType.DMA((stack,)),
            pltpu.SemaphoreType.DMA((stack,)),
        ],
        name="update",
    )(
        tile_order,
        ocean_mask.reshape(1, columns),
        obs_cell,
        window_start,
        window_span,
        obs_values,
        gain_mean,
        gain_spread,
        shared,
        levels,
    )
    return jnp.transpose(updated, (1, 0, 2))


def solution(mesh):
    in_specs = (P(None, None, ("row", "col")), P(("row", "col"))) + (P(),) * 8
    return jax.shard_map(
        per_device,
        mesh=mesh,
        in_specs=in_specs,
        out_specs=P(None, None, ("row", "col")),
        check_vma=False,
    )
```

```python
import functools
import math

import jax
import jax.numpy as jnp
from jax import lax
from jax.experimental import pallas as pl
from jax.experimental.pallas import tpu as pltpu
from jax.sharding import PartitionSpec as P

MESH = pl.DeviceIdType.MESH
NT = (((1,), (1,)), ((), ()))
SIZES = (48, 80)
SHARE_REFS = 20


def device_number():
    return lax.axis_index("row") * lax.axis_size("col") + lax.axis_index("col")


def round_up(number, step):
    return (number + step - 1) // step * step


def mate(index, step, size):
    if size & (size - 1):
        return lax.rem(index + step, size)
    bit = 1
    while bit <= step:
        if step & bit:
            index = index + bit - 2 * bit * (index // bit % 2)
        bit *= 2
    return index


def most_levels(stack, limit):
    return max(k for k in range(1, limit + 1) if stack % k == 0)


def gather_plan(gath, used, sends, receives):
    rows, cols = lax.axis_size("row"), lax.axis_size("col")
    plane = cols // 2
    row, col = lax.axis_index("row"), lax.axis_index("col")
    core, chip = lax.rem(col, 2), col // 2
    other = (row, chip * 2 + 1 - core)
    steps = [(a, b) for a in range(rows) for b in range(plane) if a or b]
    steps.sort(key=lambda step: step[0] + step[1].bit_count())
    ranked = [sorted(range(rows), key=lambda other: abs(other - here)) for here in range(rows)]

    def near_row(step):
        index = ranked[0][step]
        for here in range(1, rows):
            index = jnp.where(row == here, ranked[here][step], index)
        return index

    order = [near_row(step) for step in range(rows)]

    def place(step, twin=False):
        side = 1 - core if twin else core
        return (order[step[0]], mate(chip, step[1], plane) * 2 + side)

    def slot(step, twin):
        return order[step[0]] * cols + mate(chip, step[1], plane) * 2 + (1 - core if twin else core)

    started = []

    def send(number, to):
        copy = pltpu.make_async_remote_copy(
            src_ref=gath.at[number, 0:used],
            dst_ref=gath.at[number, 0:used],
            send_sem=sends.at[len(started)],
            recv_sem=receives.at[number],
            device_id=to,
            device_id_type=MESH,
        )
        copy.start()
        started.append(copy)

    def arrive(number):
        pltpu.make_async_remote_copy(
            src_ref=gath.at[number, 0:used],
            dst_ref=gath.at[number, 0:used],
            send_sem=sends.at[0],
            recv_sem=receives.at[number],
            device_id=other,
            device_id_type=MESH,
        ).wait_recv()

    def begin():
        mine = slot((0, 0), False)
        for step in reversed(steps):
            send(mine, place(step))
            if not step[0]:
                send(mine, place(step, True))
        send(mine, other)

    def relay():
        for step in steps:
            number = slot(step, False)
            arrive(number)
            if step[0]:
                send(number, other)

    def collect(row_step):
        for step in range(plane):
            arrive(slot((row_step, step), True))
        return order[row_step]

    def drain():
        for copy in started:
            copy.wait_send()

    twins = [place(step, True) for step in steps if not step[0]]
    return [place(step) for step in steps] + twins + [other], begin, relay, collect, drain


def share_kernel(
    round_in,
    ocean_in,
    order_in,
    order_row,
    cell_in,
    stack_in,
    x_hbm,
    *rest,
):
    extra = (len(rest) - SHARE_REFS) // 2
    ahead_in, rest = rest[:extra], rest[extra:]
    ahead_out, rest = rest[2 : 2 + extra], rest[:2] + rest[2 + extra :]
    share_body(
        (round_in, ocean_in, order_in, order_row, cell_in, stack_in, x_hbm),
        tuple(zip(ahead_in, ahead_out)),
        *rest,
    )


def share_body(
    inputs,
    handed,
    flat_ref,
    rounds_s,
    round_s,
    ocean_s,
    order_s,
    order_ref,
    cell_ref,
    stack_ref,
    xt,
    list_v,
    list_s,
    gath,
    one_hot,
    total_ref,
    sem_handed,
    sem_small,
    sem_in,
    sem_list,
    sends,
    receives,
):
    round_in, ocean_in, order_in, order_row, cell_in, stack_in, x_hbm = inputs
    stack, members, columns = x_hbm.shape
    batches, obs = cell_ref.shape
    devices, piece, lanes = gath.shape
    cap = one_hot.shape[0] // devices
    groups = columns // lanes
    parts = lanes // cap
    used = -(-(members + 1) // parts)
    me = device_number()
    state = [
        pltpu.make_async_copy(
            x_hbm.at[:, :, g * lanes : (g + 1) * lanes],
            xt.at[g * stack : (g + 1) * stack],
            sem_in.at[g],
        )
        for g in range(groups)
    ]
    pairs = (
        (order_in, order_s),
        (cell_in, cell_ref),
        (stack_in, stack_ref),
        (round_in, round_s),
        (order_row, order_ref),
        (ocean_in, ocean_s),
    )
    small = [
        pltpu.make_async_copy(source, target, sem_small.at[k])
        for k, (source, target) in enumerate(pairs)
    ]
    for copy in small + state:
        copy.start()
    peers, begin, relay, collect, drain = gather_plan(gath, used, sends, receives)
    barrier = pltpu.get_barrier_semaphore()
    for place in peers:
        pl.semaphore_signal(barrier, inc=1, device_id=place, device_id_type=MESH)
    for copy in small:
        copy.wait()

    local = cell_ref[...] - order_s[me] * columns
    here = jnp.logical_and(local >= 0, local < columns)
    ahead = here.astype(jnp.int32)
    total = ahead
    along = lax.broadcasted_iota(jnp.int32, (batches, obs), 1)
    step = 1
    while step < obs:
        ahead = ahead + jnp.where(along >= step, pltpu.roll(ahead, step, axis=1), 0)
        total = total + pltpu.roll(total, step, axis=1)
        step *= 2
    code = stack_ref[...] * columns + local
    slot_of = lax.broadcasted_iota(jnp.int32, (cap, obs), 0) + round_s[0] * cap + 1
    codes = jnp.zeros((cap, obs), jnp.int32)
    earlier = jnp.zeros((1, obs), jnp.int32)
    for b in range(batches):
        mine = jnp.where(here[b : b + 1], ahead[b : b + 1] + earlier, 0)
        codes = codes + jnp.where(mine == slot_of, code[b : b + 1], 0)
        earlier = earlier + total[b : b + 1]
    step = 1
    while step < obs:
        codes = codes + pltpu.roll(codes, step, axis=1)
        step *= 2
    diagonal = lax.broadcasted_iota(jnp.int32, (cap, obs), 0) == lax.broadcasted_iota(
        jnp.int32, (cap, obs), 1
    )
    list_v[...] = jnp.broadcast_to(
        jnp.sum(jnp.where(diagonal, codes, 0), axis=0, keepdims=True), list_v.shape
    )
    listing = pltpu.make_async_copy(list_v, list_s, sem_list)
    listing.start()

    first = (round_s[0] * cap).astype(jnp.float32)
    number = lax.broadcasted_iota(jnp.int32, (devices, obs), 0).astype(jnp.float32)
    square = (devices, devices)
    same = lax.broadcasted_iota(jnp.int32, square, 0) == lax.broadcasted_iota(jnp.int32, square, 1)
    order = jnp.sum(
        jnp.where(same, order_ref[...].astype(jnp.float32), 0.0), axis=1, keepdims=True
    )
    before = lax.broadcasted_iota(jnp.int32, (obs, obs), 0) < lax.broadcasted_iota(
        jnp.int32, (obs, obs), 1
    )
    before = before.astype(jnp.bfloat16)
    count = jnp.zeros((devices, 1), jnp.float32)
    slots = []
    for b in range(batches):
        cells = cell_ref[b : b + 1, :].astype(jnp.float32)
        tile = jnp.floor((cells + 0.5) / columns)
        holds = (order == tile).astype(jnp.float32)
        rank = count + jnp.dot(
            holds.astype(jnp.bfloat16), before, preferred_element_type=jnp.float32
        )
        count = count + jnp.sum(holds, axis=1, keepdims=True)
        rank = jnp.sum(holds * rank, axis=0, keepdims=True) - first
        holder = jnp.sum(holds * number, axis=0, keepdims=True)
        now = jnp.logical_and(rank >= 0.0, rank < cap)
        slots.append(jnp.where(now, holder * cap + rank, -1.0))
    rounds_s[0] = jnp.max(jnp.floor((count + (cap - 0.5)) / cap)).astype(jnp.int32)
    listing.wait()
    for copy in state:
        copy.wait()

    lane = lax.broadcasted_iota(jnp.int32, (members, lanes), 1)
    row8 = lax.broadcasted_iota(jnp.int32, (8, lanes), 0)
    lane8 = lax.broadcasted_iota(jnp.int32, (8, lanes), 1)

    def pick(k, carry):
        held, flags = carry
        code = list_s[0, k]
        level = lax.div(code, columns)
        local = code - level * columns
        group = lax.div(local, lanes)
        block = xt[group * stack + level]
        moved = pltpu.roll(block, lax.rem(k - (local - group * lanes) + lanes, lanes), axis=1)
        held = jnp.where(lane == k, moved, held)
        flag = jnp.where(row8 == 0, ocean_s[local].astype(jnp.float32), 0.0)
        return held, jnp.where(lane8 == k, flag, flags)

    held, flags = lax.fori_loop(
        0,
        cap,
        pick,
        (jnp.zeros((members, lanes), jnp.float32), jnp.zeros((8, lanes), jnp.float32)),
        unroll=cap,
    )
    rest = jnp.zeros((parts * piece - members, lanes), jnp.float32)
    held = jnp.concatenate([held, flags, rest], axis=0)
    part_of = lax.broadcasted_iota(jnp.int32, (piece, lanes), 1) // cap
    packed = held[0:piece]
    for g in range(1, parts):
        moved = pltpu.roll(held[g * used : g * used + piece], g * cap, axis=1)
        packed = jnp.where(part_of == g, moved, packed)
    gath[me] = packed

    pl.semaphore_wait(barrier, len(peers))
    begin()
    handed = [
        pltpu.make_async_copy(source, target, sem_handed.at[k])
        for k, (source, target) in enumerate(handed)
    ]
    for copy in handed:
        copy.start()
    at = lax.broadcasted_iota(jnp.int32, (devices * cap, obs), 0).astype(jnp.float32)
    for b in range(batches):
        one_hot[:, b * obs : (b + 1) * obs] = (slots[b] == at).astype(jnp.bfloat16)
    relay()

    rows = lax.axis_size("row")
    share = devices // rows
    for row_step in range(rows):
        row = collect(row_step)
        unpacked = []
        for g in range(parts):
            tiles = []
            for begin_at in range(0, share, parts):
                tile = None
                for q in range(parts):
                    moved = gath[row * share + begin_at + q]
                    if q != g:
                        moved = pltpu.roll(moved, (q - g) % parts * cap, axis=1)
                    tile = moved if q == 0 else jnp.where(part_of == q, moved, tile)
                tiles.append(tile)
            unpacked.append(jnp.concatenate(tiles, axis=1))
        high, low = split(jnp.concatenate(unpacked, axis=0))
        start = pl.multiple_of(row * (share * cap), share * cap)
        placed = jnp.dot(
            jnp.concatenate([high, low], axis=0),
            one_hot[pl.ds(start, share * cap), :],
            preferred_element_type=jnp.float32,
        )
        placed = placed[0 : parts * piece] + placed[parts * piece :]
        if row_step == 0:
            total_ref[...] = placed
        elif row_step < rows - 1:
            total_ref[...] += placed
        else:
            placed = total_ref[...] + placed
            placed = jnp.concatenate(
                [placed[g * piece : g * piece + used] for g in range(parts)], axis=0
            )
            for b in range(batches):
                flat_ref[b, 0 : parts * used] = placed[:, b * obs : (b + 1) * obs]
    for copy in handed:
        copy.wait()
    drain()


def split(values):
    high = values.astype(jnp.bfloat16)
    low = (values - high.astype(jnp.float32)).astype(jnp.bfloat16)
    return high, low


def triple(values, axis):
    high, low = split(values)
    return jnp.concatenate([high, low, high], axis=axis)


def product(left, right):
    high, low = split(left)
    return lax.dot_general(
        jnp.concatenate([high, high, low], axis=1),
        triple(right, 1),
        NT,
        preferred_element_type=jnp.float32,
    )


def update_kernel(
    order_s,
    ocean_ref,
    cell_ref,
    start_ref,
    span_ref,
    value_ref,
    mean_ref,
    spread_ref,
    shared_ref,
    x_hbm,
    y_hbm,
    xt,
    side_a,
    side_d,
    lhs_a,
    lhs_d,
    weight,
    held,
    sem_in,
    sem_out,
):
    stack, members, columns = xt.shape
    batches, obs = cell_ref.shape

    def incoming(v):
        return pltpu.make_async_copy(x_hbm.at[v], xt.at[v], sem_in.at[v])

    def outgoing(v):
        return pltpu.make_async_copy(xt.at[v], y_hbm.at[v], sem_out.at[v])

    def begin(v, c):
        incoming(v).start()
        return c

    lax.fori_loop(0, stack, begin, 0)

    base = (order_s[device_number()] * columns).astype(jnp.float32)
    places = base + lax.broadcasted_iota(jnp.int32, (1, columns), 1).astype(jnp.float32)
    ocean = ocean_ref[...].astype(jnp.float32)
    cells = cell_ref[...].astype(jnp.float32)
    starts = start_ref[...].astype(jnp.float32)
    ends = (start_ref[...] + span_ref[...]).astype(jnp.float32)
    priors = [shared_ref[b, 0:members, :] for b in range(batches)]
    flags = [shared_ref[b, members : members + 1, :] for b in range(batches)]
    scale = 1.0 / (members - 1.0)
    meets = jnp.logical_and(starts < base + columns, ends > base).astype(jnp.float32)
    before = lax.broadcasted_iota(jnp.int32, (obs, obs), 0) < lax.broadcasted_iota(
        jnp.int32, (obs, obs), 1
    )
    ranks = jnp.dot(
        jnp.concatenate([meets, jnp.zeros((16 - batches, obs), jnp.float32)], axis=0).astype(
            jnp.bfloat16
        ),
        before.astype(jnp.bfloat16),
        preferred_element_type=jnp.float32,
    )
    most = jnp.max(jnp.sum(meets, axis=1)).astype(jnp.int32)

    for b in range(batches):
        now = priors[b]
        centre = jnp.mean(now, axis=0, keepdims=True)
        anomalies = now - centre
        innovation = jnp.broadcast_to(value_ref[b : b + 1, :] - centre, (16, obs))
        mean_weights = product(innovation, mean_ref[b])[0:1]
        delta = mean_weights - product(anomalies, spread_ref[b])
        scaled = anomalies * scale
        high = scaled.astype(jnp.bfloat16).astype(jnp.float32)
        stacked = jnp.concatenate([high, high, scaled - high], axis=0)
        side_a[b] = stacked.astype(jnp.bfloat16)
        d_high, d_low = split(delta)
        side_d[b, 0] = d_high
        side_d[b, 1] = d_low
        if b + 1 < batches:
            start_of = jnp.transpose(jnp.broadcast_to(starts[b : b + 1], (128, obs)))[:, 0:1]
            end_of = jnp.transpose(jnp.broadcast_to(ends[b : b + 1], (128, obs)))[:, 0:1]
            later = jnp.concatenate(priors[b + 1 :], axis=1)
            cell_row = jnp.concatenate([cells[a : a + 1] for a in range(b + 1, batches)], axis=1)
            flag_row = jnp.concatenate(flags[b + 1 :], axis=1)
            inside = jnp.where(
                jnp.logical_and(cell_row >= start_of, cell_row < end_of), flag_row, 0.0
            )
            gain = inside * jnp.dot(
                jnp.transpose(stacked).astype(jnp.bfloat16),
                triple(later, 0),
                preferred_element_type=jnp.float32,
            )
            later = later + jnp.dot(
                jnp.concatenate([d_high, d_high, d_low], axis=1),
                triple(gain, 0),
                preferred_element_type=jnp.float32,
            )
            for a in range(b + 1, batches):
                priors[a] = later[:, (a - b - 1) * obs : (a - b) * obs]

    def sweep_with(kept):
        together = most_levels(stack, held.shape[0] if kept == min(SIZES) else 5)
        slot = lax.broadcasted_iota(jnp.int32, (kept, obs), 0).astype(jnp.float32)
        before_d = None
        for b in range(batches):
            chosen = jnp.logical_and(slot == ranks[b : b + 1], meets[b : b + 1] > 0.0)
            start_of = jnp.sum(jnp.where(chosen, starts[b : b + 1], 0.0), axis=1, keepdims=True)
            end_of = jnp.sum(jnp.where(chosen, ends[b : b + 1], 0.0), axis=1, keepdims=True)
            weight[b, 0:kept] = jnp.where(
                jnp.logical_and(places >= start_of, places < end_of), ocean, 0.0
            )
            pick = chosen.astype(jnp.bfloat16)
            second = b % 2
            rows = slice(second * kept, second * kept + kept)
            lhs_a[b // 2, rows] = lax.dot_general(
                pick, side_a[b], NT, preferred_element_type=jnp.float32
            ).astype(jnp.bfloat16)
            highs = lax.dot_general(side_d[b, 0], pick, NT, preferred_element_type=jnp.float32)
            lows = lax.dot_general(side_d[b, 1], pick, NT, preferred_element_type=jnp.float32)
            parts = jnp.concatenate([highs, highs, lows], axis=1).astype(jnp.bfloat16)
            lhs_d[b, 0:members, 0 : 3 * kept] = parts
            if second:
                cross = jnp.dot(
                    lhs_a[b // 2, rows],
                    before_d,
                    preferred_element_type=jnp.float32,
                )
                c_high, c_low = split(cross)
                lhs_d[b - 1, members : members + kept, 0 : 3 * kept] = jnp.concatenate([c_high, c_high, c_low], axis=1)
            else:
                before_d = jnp.concatenate([highs, lows, highs], axis=0).astype(jnp.bfloat16)

        def sweep(number, c):
            levels = [number * together + k for k in range(together)]
            for v in levels:
                incoming(v).wait()
            values = [xt[v] for v in levels]
            for b in range(0, batches, 2):
                both = []
                for k in range(together):
                    both.append(
                        jnp.dot(
                            lhs_a[b // 2, 0 : 2 * kept],
                            triple(values[k], 0),
                            preferred_element_type=jnp.float32,
                        )
                    )
                for k in range(together):
                    held[k, 0:kept] = both[k][kept:]
                moved = []
                for k in range(together):
                    gain = triple(weight[b, 0:kept] * both[k][0:kept], 0)
                    moved.append(
                        jnp.dot(
                            lhs_d[b, 0 : kept + members, 0 : 3 * kept],
                            gain,
                            preferred_element_type=jnp.float32,
                        )
                    )
                for k in range(together):
                    xt[levels[k]] = values[k] + moved[k][0:members]
                for k in range(together):
                    gain = weight[b + 1, 0:kept] * (held[k, 0:kept] + moved[k][members:])
                    values[k] = (
                        xt[levels[k]]
                        + jnp.dot(
                            lhs_d[b + 1, 0:members, 0 : 3 * kept],
                            triple(gain, 0),
                            preferred_element_type=jnp.float32,
                        )
                    )
            for k in range(together):
                xt[levels[k]] = values[k]
            for v in levels:
                outgoing(v).start()
            return c

        lax.fori_loop(0, stack // together, sweep, 0)

    sizes = [kept for kept in SIZES if kept < obs] + [obs]
    for low, kept in zip([-1] + sizes[:-1], sizes):
        pl.when(jnp.logical_and(most > low, most <= kept))(functools.partial(sweep_with, kept))

    def end(v, c):
        outgoing(v).wait()
        return c

    lax.fori_loop(0, stack, end, 0)


def per_device(
    prior,
    ocean_mask,
    tile_order,
    obs_cell,
    obs_stack,
    obs_values,
    window_start,
    window_span,
    gain_mean,
    gain_spread,
):
    members, stack, columns = prior.shape
    batches, obs = obs_cell.shape
    devices = tile_order.shape[0]
    mean = -(-batches * obs // devices)
    cap = 8
    while cap < min(mean + 4 * math.isqrt(mean), 128):
        cap *= 2
    parts = 128 // cap
    piece = round_up(-(-(members + 1) // parts), 8)
    smem = pl.BlockSpec(memory_space=pltpu.SMEM)
    vmem = pl.BlockSpec(memory_space=pltpu.VMEM)
    hbm = pl.BlockSpec(memory_space=pl.ANY)

    levels = jnp.transpose(prior, (1, 0, 2))

    ahead = (window_start, window_span, obs_values, gain_mean, gain_spread)

    def share(number):
        return pl.pallas_call(
            share_kernel,
            out_shape=(
                jax.ShapeDtypeStruct((batches, parts * piece, obs), jnp.float32),
                jax.ShapeDtypeStruct((1,), jnp.int32),
            )
            + tuple(jax.ShapeDtypeStruct(array.shape, array.dtype) for array in ahead),
            in_specs=[hbm] * (7 + len(ahead)),
            out_specs=(vmem, smem) + (vmem,) * len(ahead),
            scratch_shapes=[
                pltpu.SMEM((1,), jnp.int32),
                pltpu.SMEM((columns,), jnp.int32),
                pltpu.SMEM((devices,), jnp.int32),
                pltpu.VMEM((1, devices), jnp.int32),
                pltpu.VMEM((batches, obs), jnp.int32),
                pltpu.VMEM((batches, obs), jnp.int32),
                pltpu.VMEM((columns // 128 * stack, members, 128), jnp.float32),
                pltpu.VMEM((1, obs), jnp.int32),
                pltpu.SMEM((1, obs), jnp.int32),
                pltpu.VMEM((devices, piece, 128), jnp.float32),
                pltpu.VMEM((devices * cap, batches * obs), jnp.bfloat16),
                pltpu.VMEM((parts * piece, batches * obs), jnp.float32),
                pltpu.SemaphoreType.DMA((max(len(ahead), 1),)),
                pltpu.SemaphoreType.DMA((6,)),
                pltpu.SemaphoreType.DMA((columns // 128,)),
                pltpu.SemaphoreType.DMA,
                pltpu.SemaphoreType.DMA((devices,)),
                pltpu.SemaphoreType.DMA((devices,)),
            ],
            compiler_params=pltpu.CompilerParams(
                collective_id=0, has_side_effects=True, vmem_limit_bytes=24 * 2**20
            ),
            name="share",
        )(number, ocean_mask, tile_order, tile_order.reshape(1, devices), obs_cell, obs_stack, levels, *ahead)

    shared, rounds, *handed = share(jnp.zeros((1,), jnp.int32))
    _, shared = lax.while_loop(
        lambda carry: carry[0] < rounds[0],
        lambda carry: (carry[0] + 1, carry[1] + share(carry[0].reshape(1))[0]),
        (jnp.int32(1), shared),
    )

    updated = pl.pallas_call(
        update_kernel,
        out_shape=jax.ShapeDtypeStruct(levels.shape, levels.dtype),
        in_specs=[smem] + [vmem] * 8 + [hbm],
        out_specs=hbm,
        scratch_shapes=[
            pltpu.VMEM((stack, members, columns), jnp.float32),
            pltpu.VMEM((batches, 3 * members, obs), jnp.bfloat16),
            pltpu.VMEM((batches, 2, members, obs), jnp.bfloat16),
            pltpu.VMEM((batches // 2, 2 * obs, 3 * members), jnp.bfloat16),
            pltpu.VMEM((batches, members + obs, 3 * obs), jnp.bfloat16),
            pltpu.VMEM((batches, obs, columns), jnp.float32),
            pltpu.VMEM((most_levels(stack, 10), obs, columns), jnp.float32),
            pltpu.SemaphoreType.DMA((stack,)),
            pltpu.SemaphoreType.DMA((stack,)),
        ],
        compiler_params=pltpu.CompilerParams(vmem_limit_bytes=32 * 2**20),
        name="update",
    )(
        tile_order,
        ocean_mask.reshape(1, columns),
        obs_cell,
        *handed,
        shared,
        levels,
    )
    return jnp.transpose(updated, (1, 0, 2))


def solution(mesh):
    in_specs = (P(None, None, ("row", "col")), P(("row", "col"))) + (P(),) * 8
    return jax.shard_map(
        per_device,
        mesh=mesh,
        in_specs=in_specs,
        out_specs=P(None, None, ("row", "col")),
        check_vma=False,
    )
```

```python
import functools
import math

import jax
import jax.numpy as jnp
from jax import lax
from jax.experimental import pallas as pl
from jax.experimental.pallas import tpu as pltpu
from jax.sharding import PartitionSpec as P

MESH = pl.DeviceIdType.MESH
NT = (((1,), (1,)), ((), ()))
SIZES = (48, 80)
SHARE_REFS = 20


def device_number():
    return lax.axis_index("row") * lax.axis_size("col") + lax.axis_index("col")


def round_up(number, step):
    return (number + step - 1) // step * step


def mate(index, step, size):
    if size & (size - 1):
        return lax.rem(index + step, size)
    bit = 1
    while bit <= step:
        if step & bit:
            index = index + bit - 2 * bit * (index // bit % 2)
        bit *= 2
    return index


def most_levels(stack, limit):
    return max(k for k in range(1, limit + 1) if stack % k == 0)


def gather_plan(gath, used, sends, receives):
    rows, cols = lax.axis_size("row"), lax.axis_size("col")
    plane = cols // 2
    row, col = lax.axis_index("row"), lax.axis_index("col")
    core, chip = lax.rem(col, 2), col // 2
    other = (row, chip * 2 + 1 - core)
    steps = [(a, b) for a in range(rows) for b in range(plane) if a or b]
    steps.sort(key=lambda step: step[0] + step[1].bit_count())
    ranked = [sorted(range(rows), key=lambda other: abs(other - here)) for here in range(rows)]

    def near_row(step):
        index = ranked[0][step]
        for here in range(1, rows):
            index = jnp.where(row == here, ranked[here][step], index)
        return index

    order = [near_row(step) for step in range(rows)]

    def place(step, twin=False):
        side = 1 - core if twin else core
        return (order[step[0]], mate(chip, step[1], plane) * 2 + side)

    def slot(step, twin):
        return order[step[0]] * cols + mate(chip, step[1], plane) * 2 + (1 - core if twin else core)

    started = []

    def send(number, to):
        copy = pltpu.make_async_remote_copy(
            src_ref=gath.at[number, 0:used],
            dst_ref=gath.at[number, 0:used],
            send_sem=sends.at[len(started)],
            recv_sem=receives.at[number],
            device_id=to,
            device_id_type=MESH,
        )
        copy.start()
        started.append(copy)

    def arrive(number):
        pltpu.make_async_remote_copy(
            src_ref=gath.at[number, 0:used],
            dst_ref=gath.at[number, 0:used],
            send_sem=sends.at[0],
            recv_sem=receives.at[number],
            device_id=other,
            device_id_type=MESH,
        ).wait_recv()

    def begin():
        mine = slot((0, 0), False)
        for step in reversed(steps):
            send(mine, place(step))
            if not step[0]:
                send(mine, place(step, True))
        send(mine, other)

    def relay():
        for step in steps:
            number = slot(step, False)
            arrive(number)
            if step[0]:
                send(number, other)

    def collect(row_step):
        for step in range(plane):
            arrive(slot((row_step, step), True))
        return order[row_step]

    def drain():
        for copy in started:
            copy.wait_send()

    twins = [place(step, True) for step in steps if not step[0]]
    return [place(step) for step in steps] + twins + [other], begin, relay, collect, drain


def share_kernel(
    round_in,
    ocean_in,
    order_in,
    order_row,
    cell_in,
    stack_in,
    x_hbm,
    *rest,
):
    extra = (len(rest) - SHARE_REFS) // 2
    ahead_in, rest = rest[:extra], rest[extra:]
    ahead_out, rest = rest[2 : 2 + extra], rest[:2] + rest[2 + extra :]
    share_body(
        (round_in, ocean_in, order_in, order_row, cell_in, stack_in, x_hbm),
        tuple(zip(ahead_in, ahead_out)),
        *rest,
    )


def share_body(
    inputs,
    handed,
    flat_ref,
    rounds_s,
    round_s,
    ocean_s,
    order_s,
    order_ref,
    cell_ref,
    stack_ref,
    xt,
    list_v,
    list_s,
    gath,
    one_hot,
    total_ref,
    sem_handed,
    sem_small,
    sem_in,
    sem_list,
    sends,
    receives,
):
    round_in, ocean_in, order_in, order_row, cell_in, stack_in, x_hbm = inputs
    stack, members, columns = x_hbm.shape
    batches, obs = cell_ref.shape
    devices, piece, lanes = gath.shape
    cap = one_hot.shape[0] // devices
    groups = columns // lanes
    parts = lanes // cap
    used = -(-(members + 1) // parts)
    me = device_number()
    state = [
        pltpu.make_async_copy(
            x_hbm.at[:, :, g * lanes : (g + 1) * lanes],
            xt.at[g * stack : (g + 1) * stack],
            sem_in.at[g],
        )
        for g in range(groups)
    ]
    pairs = (
        (order_in, order_s),
        (cell_in, cell_ref),
        (stack_in, stack_ref),
        (round_in, round_s),
        (order_row, order_ref),
        (ocean_in, ocean_s),
    )
    small = [
        pltpu.make_async_copy(source, target, sem_small.at[k])
        for k, (source, target) in enumerate(pairs)
    ]
    for copy in small + state:
        copy.start()
    peers, begin, relay, collect, drain = gather_plan(gath, used, sends, receives)
    barrier = pltpu.get_barrier_semaphore()
    for place in peers:
        pl.semaphore_signal(barrier, inc=1, device_id=place, device_id_type=MESH)
    for copy in small:
        copy.wait()

    local = cell_ref[...] - order_s[me] * columns
    here = jnp.logical_and(local >= 0, local < columns)
    ahead = here.astype(jnp.int32)
    total = ahead
    along = lax.broadcasted_iota(jnp.int32, (batches, obs), 1)
    step = 1
    while step < obs:
        ahead = ahead + jnp.where(along >= step, pltpu.roll(ahead, step, axis=1), 0)
        total = total + pltpu.roll(total, step, axis=1)
        step *= 2
    code = stack_ref[...] * columns + local
    slot_of = lax.broadcasted_iota(jnp.int32, (cap, obs), 0) + round_s[0] * cap + 1
    codes = jnp.zeros((cap, obs), jnp.int32)
    earlier = jnp.zeros((1, obs), jnp.int32)
    for b in range(batches):
        mine = jnp.where(here[b : b + 1], ahead[b : b + 1] + earlier, 0)
        codes = codes + jnp.where(mine == slot_of, code[b : b + 1], 0)
        earlier = earlier + total[b : b + 1]
    step = 1
    while step < obs:
        codes = codes + pltpu.roll(codes, step, axis=1)
        step *= 2
    diagonal = lax.broadcasted_iota(jnp.int32, (cap, obs), 0) == lax.broadcasted_iota(
        jnp.int32, (cap, obs), 1
    )
    list_v[...] = jnp.broadcast_to(
        jnp.sum(jnp.where(diagonal, codes, 0), axis=0, keepdims=True), list_v.shape
    )
    listing = pltpu.make_async_copy(list_v, list_s, sem_list)
    listing.start()

    first = (round_s[0] * cap).astype(jnp.float32)
    number = lax.broadcasted_iota(jnp.int32, (devices, obs), 0).astype(jnp.float32)
    square = (devices, devices)
    same = lax.broadcasted_iota(jnp.int32, square, 0) == lax.broadcasted_iota(jnp.int32, square, 1)
    order = jnp.sum(
        jnp.where(same, order_ref[...].astype(jnp.float32), 0.0), axis=1, keepdims=True
    )
    before = lax.broadcasted_iota(jnp.int32, (obs, obs), 0) < lax.broadcasted_iota(
        jnp.int32, (obs, obs), 1
    )
    before = before.astype(jnp.bfloat16)
    count = jnp.zeros((devices, 1), jnp.float32)
    slots = []
    for b in range(batches):
        cells = cell_ref[b : b + 1, :].astype(jnp.float32)
        tile = jnp.floor((cells + 0.5) / columns)
        holds = (order == tile).astype(jnp.float32)
        rank = count + jnp.dot(
            holds.astype(jnp.bfloat16), before, preferred_element_type=jnp.float32
        )
        count = count + jnp.sum(holds, axis=1, keepdims=True)
        rank = jnp.sum(holds * rank, axis=0, keepdims=True) - first
        holder = jnp.sum(holds * number, axis=0, keepdims=True)
        now = jnp.logical_and(rank >= 0.0, rank < cap)
        slots.append(jnp.where(now, holder * cap + rank, -1.0))
    rounds_s[0] = jnp.max(jnp.floor((count + (cap - 0.5)) / cap)).astype(jnp.int32)
    listing.wait()
    for copy in state:
        copy.wait()

    lane = lax.broadcasted_iota(jnp.int32, (members, lanes), 1)
    row8 = lax.broadcasted_iota(jnp.int32, (8, lanes), 0)
    lane8 = lax.broadcasted_iota(jnp.int32, (8, lanes), 1)

    def pick(k, carry):
        held, flags = carry
        code = list_s[0, k]
        level = lax.div(code, columns)
        local = code - level * columns
        group = lax.div(local, lanes)
        block = xt[group * stack + level]
        moved = pltpu.roll(block, lax.rem(k - (local - group * lanes) + lanes, lanes), axis=1)
        held = jnp.where(lane == k, moved, held)
        flag = jnp.where(row8 == 0, ocean_s[local].astype(jnp.float32), 0.0)
        return held, jnp.where(lane8 == k, flag, flags)

    held, flags = lax.fori_loop(
        0,
        cap,
        pick,
        (jnp.zeros((members, lanes), jnp.float32), jnp.zeros((8, lanes), jnp.float32)),
        unroll=cap,
    )
    rest = jnp.zeros((parts * piece - members, lanes), jnp.float32)
    held = jnp.concatenate([held, flags, rest], axis=0)
    part_of = lax.broadcasted_iota(jnp.int32, (piece, lanes), 1) // cap
    packed = held[0:piece]
    for g in range(1, parts):
        moved = pltpu.roll(held[g * used : g * used + piece], g * cap, axis=1)
        packed = jnp.where(part_of == g, moved, packed)
    gath[me] = packed

    pl.semaphore_wait(barrier, len(peers))
    begin()
    handed = [
        pltpu.make_async_copy(source, target, sem_handed.at[k])
        for k, (source, target) in enumerate(handed)
    ]
    for copy in handed:
        copy.start()
    at = lax.broadcasted_iota(jnp.int32, (devices * cap, obs), 0).astype(jnp.float32)
    for b in range(batches):
        one_hot[:, b * obs : (b + 1) * obs] = (slots[b] == at).astype(jnp.bfloat16)
    relay()

    rows = lax.axis_size("row")
    share = devices // rows
    for row_step in range(rows):
        row = collect(row_step)
        unpacked = []
        for g in range(parts):
            tiles = []
            for begin_at in range(0, share, parts):
                tile = None
                for q in range(parts):
                    moved = gath[row * share + begin_at + q]
                    if q != g:
                        moved = pltpu.roll(moved, (q - g) % parts * cap, axis=1)
                    tile = moved if q == 0 else jnp.where(part_of == q, moved, tile)
                tiles.append(tile)
            unpacked.append(jnp.concatenate(tiles, axis=1))
        high, low = split(jnp.concatenate(unpacked, axis=0))
        start = pl.multiple_of(row * (share * cap), share * cap)
        placed = jnp.dot(
            jnp.concatenate([high, low], axis=0),
            one_hot[pl.ds(start, share * cap), :],
            preferred_element_type=jnp.float32,
        )
        placed = placed[0 : parts * piece] + placed[parts * piece :]
        if row_step == 0:
            total_ref[...] = placed
        elif row_step < rows - 1:
            total_ref[...] += placed
        else:
            placed = total_ref[...] + placed
            placed = jnp.concatenate(
                [placed[g * piece : g * piece + used] for g in range(parts)], axis=0
            )
            for b in range(batches):
                flat_ref[b, 0 : parts * used] = placed[:, b * obs : (b + 1) * obs]
    for copy in handed:
        copy.wait()
    drain()


def split(values):
    high = values.astype(jnp.bfloat16)
    low = (values - high.astype(jnp.float32)).astype(jnp.bfloat16)
    return high, low


def triple(values, axis):
    high, low = split(values)
    return jnp.concatenate([high, low, high], axis=axis)


def product(left, right):
    high, low = split(left)
    return lax.dot_general(
        jnp.concatenate([high, high, low], axis=1),
        triple(right, 1),
        NT,
        preferred_element_type=jnp.float32,
    )


def update_kernel(
    order_s,
    ocean_ref,
    cell_ref,
    start_ref,
    span_ref,
    value_ref,
    mean_ref,
    spread_ref,
    shared_ref,
    x_hbm,
    y_hbm,
    xt,
    side_a,
    side_d,
    lhs_a,
    lhs_d,
    weight,
    held,
    sem_in,
    sem_out,
):
    stack, members, columns = xt.shape
    batches, obs = cell_ref.shape

    def incoming(v):
        return pltpu.make_async_copy(x_hbm.at[v], xt.at[v], sem_in.at[v])

    def outgoing(v):
        return pltpu.make_async_copy(xt.at[v], y_hbm.at[v], sem_out.at[v])

    def begin(v, c):
        incoming(v).start()
        return c

    lax.fori_loop(0, stack, begin, 0)

    base = (order_s[device_number()] * columns).astype(jnp.float32)
    places = base + lax.broadcasted_iota(jnp.int32, (1, columns), 1).astype(jnp.float32)
    ocean = ocean_ref[...].astype(jnp.float32)
    cells = cell_ref[...].astype(jnp.float32)
    starts = start_ref[...].astype(jnp.float32)
    ends = (start_ref[...] + span_ref[...]).astype(jnp.float32)
    priors = [shared_ref[b, 0:members, :] for b in range(batches)]
    flags = [shared_ref[b, members : members + 1, :] for b in range(batches)]
    scale = 1.0 / (members - 1.0)
    meets = jnp.logical_and(starts < base + columns, ends > base).astype(jnp.float32)
    before = lax.broadcasted_iota(jnp.int32, (obs, obs), 0) < lax.broadcasted_iota(
        jnp.int32, (obs, obs), 1
    )
    ranks = jnp.dot(
        jnp.concatenate([meets, jnp.zeros((16 - batches, obs), jnp.float32)], axis=0).astype(
            jnp.bfloat16
        ),
        before.astype(jnp.bfloat16),
        preferred_element_type=jnp.float32,
    )
    most = jnp.max(jnp.sum(meets, axis=1)).astype(jnp.int32)

    for b in range(batches):
        now = priors[b]
        centre = jnp.mean(now, axis=0, keepdims=True)
        anomalies = now - centre
        innovation = jnp.broadcast_to(value_ref[b : b + 1, :] - centre, (16, obs))
        mean_weights = product(innovation, mean_ref[b])[0:1]
        delta = mean_weights - product(anomalies, spread_ref[b])
        scaled = anomalies * scale
        high = scaled.astype(jnp.bfloat16).astype(jnp.float32)
        stacked = jnp.concatenate([high, high, scaled - high], axis=0)
        side_a[b] = stacked.astype(jnp.bfloat16)
        d_high, d_low = split(delta)
        side_d[b, 0] = d_high
        side_d[b, 1] = d_low
        if b + 1 < batches:
            start_of = jnp.transpose(jnp.broadcast_to(starts[b : b + 1], (128, obs)))[:, 0:1]
            end_of = jnp.transpose(jnp.broadcast_to(ends[b : b + 1], (128, obs)))[:, 0:1]
            later = jnp.concatenate(priors[b + 1 :], axis=1)
            cell_row = jnp.concatenate([cells[a : a + 1] for a in range(b + 1, batches)], axis=1)
            flag_row = jnp.concatenate(flags[b + 1 :], axis=1)
            inside = jnp.where(
                jnp.logical_and(cell_row >= start_of, cell_row < end_of), flag_row, 0.0
            )
            gain = inside * jnp.dot(
                jnp.transpose(stacked).astype(jnp.bfloat16),
                triple(later, 0),
                preferred_element_type=jnp.float32,
            )
            later = later + jnp.dot(
                jnp.concatenate([d_high, d_high, d_low], axis=1),
                triple(gain, 0),
                preferred_element_type=jnp.float32,
            )
            for a in range(b + 1, batches):
                priors[a] = later[:, (a - b - 1) * obs : (a - b) * obs]

    def sweep_with(kept):
        together = most_levels(stack, held.shape[0] if kept == min(SIZES) else 5)
        slot = lax.broadcasted_iota(jnp.int32, (kept, obs), 0).astype(jnp.float32)
        before_d = None
        for b in range(batches):
            chosen = jnp.logical_and(slot == ranks[b : b + 1], meets[b : b + 1] > 0.0)
            start_of = jnp.sum(jnp.where(chosen, starts[b : b + 1], 0.0), axis=1, keepdims=True)
            end_of = jnp.sum(jnp.where(chosen, ends[b : b + 1], 0.0), axis=1, keepdims=True)
            weight[b, 0:kept] = jnp.where(
                jnp.logical_and(places >= start_of, places < end_of), ocean, 0.0
            )
            pick = chosen.astype(jnp.bfloat16)
            second = b % 2
            rows = slice(second * kept, second * kept + kept)
            lhs_a[b // 2, rows] = lax.dot_general(
                pick, side_a[b], NT, preferred_element_type=jnp.float32
            ).astype(jnp.bfloat16)
            highs = lax.dot_general(side_d[b, 0], pick, NT, preferred_element_type=jnp.float32)
            lows = lax.dot_general(side_d[b, 1], pick, NT, preferred_element_type=jnp.float32)
            parts = jnp.concatenate([highs, highs, lows], axis=1).astype(jnp.bfloat16)
            lhs_d[b, 0:members, 0 : 3 * kept] = parts
            if kept == obs:
                continue
            if second:
                cross = jnp.dot(
                    lhs_a[b // 2, rows],
                    before_d,
                    preferred_element_type=jnp.float32,
                )
                c_high, c_low = split(cross)
                lhs_d[b - 1, members : members + kept, 0 : 3 * kept] = jnp.concatenate([c_high, c_high, c_low], axis=1)
            else:
                before_d = jnp.concatenate([highs, lows, highs], axis=0).astype(jnp.bfloat16)

        def sweep(number, c):
            levels = [number * together + k for k in range(together)]
            for v in levels:
                incoming(v).wait()
            values = [xt[v] for v in levels]
            for b in range(batches if kept == obs else 0):
                gains = []
                for k in range(together):
                    gain = weight[b] * jnp.dot(
                        lhs_a[b // 2, b % 2 * obs : b % 2 * obs + obs],
                        triple(values[k], 0),
                        preferred_element_type=jnp.float32,
                    )
                    gains.append(triple(gain, 0))
                for k in range(together):
                    values[k] = values[k] + jnp.dot(
                        lhs_d[b, 0:members], gains[k], preferred_element_type=jnp.float32
                    )
            for b in range(0, batches if kept < obs else 0, 2):
                both = []
                for k in range(together):
                    both.append(
                        jnp.dot(
                            lhs_a[b // 2, 0 : 2 * kept],
                            triple(values[k], 0),
                            preferred_element_type=jnp.float32,
                        )
                    )
                for k in range(together):
                    held[k, 0:kept] = both[k][kept:]
                moved = []
                for k in range(together):
                    gain = triple(weight[b, 0:kept] * both[k][0:kept], 0)
                    moved.append(
                        jnp.dot(
                            lhs_d[b, 0 : kept + members, 0 : 3 * kept],
                            gain,
                            preferred_element_type=jnp.float32,
                        )
                    )
                for k in range(together):
                    xt[levels[k]] = values[k] + moved[k][0:members]
                for k in range(together):
                    gain = weight[b + 1, 0:kept] * (held[k, 0:kept] + moved[k][members:])
                    values[k] = (
                        xt[levels[k]]
                        + jnp.dot(
                            lhs_d[b + 1, 0:members, 0 : 3 * kept],
                            triple(gain, 0),
                            preferred_element_type=jnp.float32,
                        )
                    )
            for k in range(together):
                xt[levels[k]] = values[k]
            for v in levels:
                outgoing(v).start()
            return c

        lax.fori_loop(0, stack // together, sweep, 0)

    sizes = [kept for kept in SIZES if kept < obs] + [obs]
    for low, kept in zip([-1] + sizes[:-1], sizes):
        pl.when(jnp.logical_and(most > low, most <= kept))(functools.partial(sweep_with, kept))

    def end(v, c):
        outgoing(v).wait()
        return c

    lax.fori_loop(0, stack, end, 0)


def per_device(
    prior,
    ocean_mask,
    tile_order,
    obs_cell,
    obs_stack,
    obs_values,
    window_start,
    window_span,
    gain_mean,
    gain_spread,
):
    members, stack, columns = prior.shape
    batches, obs = obs_cell.shape
    devices = tile_order.shape[0]
    mean = -(-batches * obs // devices)
    cap = 8
    while cap < min(mean + 4 * math.isqrt(mean), 128):
        cap *= 2
    parts = 128 // cap
    piece = round_up(-(-(members + 1) // parts), 8)
    smem = pl.BlockSpec(memory_space=pltpu.SMEM)
    vmem = pl.BlockSpec(memory_space=pltpu.VMEM)
    hbm = pl.BlockSpec(memory_space=pl.ANY)

    levels = jnp.transpose(prior, (1, 0, 2))

    ahead = (window_start, window_span, obs_values, gain_mean, gain_spread)

    def share(number):
        return pl.pallas_call(
            share_kernel,
            out_shape=(
                jax.ShapeDtypeStruct((batches, parts * piece, obs), jnp.float32),
                jax.ShapeDtypeStruct((1,), jnp.int32),
            )
            + tuple(jax.ShapeDtypeStruct(array.shape, array.dtype) for array in ahead),
            in_specs=[hbm] * (7 + len(ahead)),
            out_specs=(vmem, smem) + (vmem,) * len(ahead),
            scratch_shapes=[
                pltpu.SMEM((1,), jnp.int32),
                pltpu.SMEM((columns,), jnp.int32),
                pltpu.SMEM((devices,), jnp.int32),
                pltpu.VMEM((1, devices), jnp.int32),
                pltpu.VMEM((batches, obs), jnp.int32),
                pltpu.VMEM((batches, obs), jnp.int32),
                pltpu.VMEM((columns // 128 * stack, members, 128), jnp.float32),
                pltpu.VMEM((1, obs), jnp.int32),
                pltpu.SMEM((1, obs), jnp.int32),
                pltpu.VMEM((devices, piece, 128), jnp.float32),
                pltpu.VMEM((devices * cap, batches * obs), jnp.bfloat16),
                pltpu.VMEM((parts * piece, batches * obs), jnp.float32),
                pltpu.SemaphoreType.DMA((max(len(ahead), 1),)),
                pltpu.SemaphoreType.DMA((6,)),
                pltpu.SemaphoreType.DMA((columns // 128,)),
                pltpu.SemaphoreType.DMA,
                pltpu.SemaphoreType.DMA((devices,)),
                pltpu.SemaphoreType.DMA((devices,)),
            ],
            compiler_params=pltpu.CompilerParams(
                collective_id=0, has_side_effects=True, vmem_limit_bytes=24 * 2**20
            ),
            name="share",
        )(number, ocean_mask, tile_order, tile_order.reshape(1, devices), obs_cell, obs_stack, levels, *ahead)

    shared, rounds, *handed = share(jnp.zeros((1,), jnp.int32))
    _, shared = lax.while_loop(
        lambda carry: carry[0] < rounds[0],
        lambda carry: (carry[0] + 1, carry[1] + share(carry[0].reshape(1))[0]),
        (jnp.int32(1), shared),
    )

    updated = pl.pallas_call(
        update_kernel,
        out_shape=jax.ShapeDtypeStruct(levels.shape, levels.dtype),
        in_specs=[smem] + [vmem] * 8 + [hbm],
        out_specs=hbm,
        scratch_shapes=[
            pltpu.VMEM((stack, members, columns), jnp.float32),
            pltpu.VMEM((batches, 3 * members, obs), jnp.bfloat16),
            pltpu.VMEM((batches, 2, members, obs), jnp.bfloat16),
            pltpu.VMEM((batches // 2, 2 * obs, 3 * members), jnp.bfloat16),
            pltpu.VMEM((batches, members + obs, 3 * obs), jnp.bfloat16),
            pltpu.VMEM((batches, obs, columns), jnp.float32),
            pltpu.VMEM((most_levels(stack, 10), obs, columns), jnp.float32),
            pltpu.SemaphoreType.DMA((stack,)),
            pltpu.SemaphoreType.DMA((stack,)),
        ],
        compiler_params=pltpu.CompilerParams(vmem_limit_bytes=32 * 2**20),
        name="update",
    )(
        tile_order,
        ocean_mask.reshape(1, columns),
        obs_cell,
        *handed,
        shared,
        levels,
    )
    return jnp.transpose(updated, (1, 0, 2))


def solution(mesh):
    in_specs = (P(None, None, ("row", "col")), P(("row", "col"))) + (P(),) * 8
    return jax.shard_map(
        per_device,
        mesh=mesh,
        in_specs=in_specs,
        out_specs=P(None, None, ("row", "col")),
        check_vma=False,
    )
```
